8 devices in a mesh: dp: 1 (over z), tp2: 2 (over y), tp: 4 (over x, core).
Axes of the slice: x: 2, y: 2, z: 1, core: 2. Of those that a mesh axis runs over, the one named last changes fastest.
Arguments:
- hidden: bfloat16 [1024, 4096], P('dp')
- w_gate: bfloat16 [4096, 11008], P(None, ('tp2', 'tp'))
- w_up: bfloat16 [4096, 11008], P(None, ('tp2', 'tp'))
- w_down: bfloat16 [11008, 4096], P(('tp2', 'tp'))
- norm_gain: float32 [4096], replicated
- w_vocab: bfloat16 [4096, 32000], P(None, ('tp2', 'tp'))
- temperature: float32 [1024], P('dp')
- target_ids: int32 [1024], P('dp')
Outputs:
- output 1: float32 [1024], P('dp')
- output 2: float32 [1024], P('dp')
- output 3: float32 [1024], P('dp')
- output 4: bfloat16 [1024, 32000], P('dp', ('tp2', 'tp'))
All inputs are finite; a program needn't handle non-finite values.
Results may differ from the reference program's by a relative error of at most 0.00376407.
Values are sent between devices in bfloat16 or wider.
A program may use at most 1 GiB of HBM per device.

```python
import jax
import jax.numpy as jnp
from jax import lax

BATCH_ROWS = 1024
D_MODEL = 4096
D_FF = 11008
VOCAB_SIZE = 32000
ROW_BLOCK = 8
NORM_EPS = 1e-6


def setup_inputs(seed: int = 0, part: int = 0) -> dict:
    base_key = jax.random.key(seed)
    part_key = jax.random.fold_in(base_key, part)
    shared = jax.random.split(base_key, 6)
    own_keys = jax.random.split(part_key, 3)
    hidden = jax.random.normal(own_keys[0], (BATCH_ROWS, D_MODEL), jnp.float32)
    w_gate = jax.random.normal(shared[0], (D_MODEL, D_FF), jnp.float32) * D_MODEL ** -0.5
    w_up = jax.random.normal(shared[1], (D_MODEL, D_FF), jnp.float32) * D_MODEL ** -0.5
    w_down = jax.random.normal(shared[2], (D_FF, D_MODEL), jnp.float32) * (2.0 * D_FF ** -0.5)
    norm_gain = jax.random.uniform(shared[3], (D_MODEL,), jnp.float32, 0.5, 1.5)
    col_scale = jnp.exp(0.3 * jax.random.normal(shared[4], (1, VOCAB_SIZE), jnp.float32))
    w_vocab = jax.random.normal(shared[5], (D_MODEL, VOCAB_SIZE), jnp.float32) * D_MODEL ** -0.5 * col_scale
    temperature = jax.random.uniform(own_keys[1], (BATCH_ROWS,), jnp.float32, 0.5, 2.0)
    target_ids = jax.random.randint(own_keys[2], (BATCH_ROWS,), 0, VOCAB_SIZE, jnp.int32)
    return {
        'hidden': hidden.astype(jnp.bfloat16),
        'w_gate': w_gate.astype(jnp.bfloat16),
        'w_up': w_up.astype(jnp.bfloat16),
        'w_down': w_down.astype(jnp.bfloat16),
        'norm_gain': norm_gain,
        'w_vocab': w_vocab.astype(jnp.bfloat16),
        'temperature': temperature,
        'target_ids': target_ids,
    }


def reference(hidden, w_gate, w_up, w_down, norm_gain, w_vocab, temperature, target_ids):
    gate_pre = jnp.dot(hidden, w_gate, preferred_element_type=jnp.float32)
    up_pre = jnp.dot(hidden, w_up, preferred_element_type=jnp.float32)
    hidden_act = (jax.nn.silu(gate_pre) * up_pre).astype(jnp.bfloat16)
    mlp_out = jnp.dot(hidden_act, w_down, preferred_element_type=jnp.float32).astype(jnp.bfloat16)
    resid_sum = hidden.astype(jnp.float32) + mlp_out.astype(jnp.float32)
    inv_rms = lax.rsqrt(jnp.mean(resid_sum * resid_sum, axis=-1, keepdims=True) + NORM_EPS)
    normed = (norm_gain * resid_sum * inv_rms).astype(jnp.bfloat16)
    num_blocks = BATCH_ROWS // ROW_BLOCK

    def head_block(block_in):
        block_x, block_temp, block_ids = block_in
        logits = jnp.dot(block_x, w_vocab, preferred_element_type=jnp.float32) / block_temp[:, None]
        row_max = jnp.max(logits, axis=-1, keepdims=True)
        shifted = jnp.exp(logits - row_max)
        sum_exp = jnp.sum(shifted, axis=-1)
        log_norm = row_max[:, 0] + jnp.log(sum_exp)
        mean_logit = jnp.sum(shifted * logits, axis=-1) / sum_exp
        target_logit = jnp.take_along_axis(logits, block_ids[:, None], axis=-1)[:, 0]
        logprobs = (logits - log_norm[:, None]).astype(jnp.bfloat16)
        return log_norm, log_norm - mean_logit, target_logit - log_norm, logprobs

    log_norm, entropy, target_logp, logprobs = lax.map(
        head_block,
        (normed.reshape(num_blocks, ROW_BLOCK, D_MODEL),
         temperature.reshape(num_blocks, ROW_BLOCK),
         target_ids.reshape(num_blocks, ROW_BLOCK)))
    return (log_norm.reshape(BATCH_ROWS), entropy.reshape(BATCH_ROWS),
            target_logp.reshape(BATCH_ROWS), logprobs.reshape(BATCH_ROWS, VOCAB_SIZE))
```

```python
import jax
import jax.numpy as jnp
from jax import lax
from jax.experimental import pallas as pl
from jax.experimental.pallas import tpu as pltpu
from jax.sharding import PartitionSpec as P

NORM_EPS = 1e-6
ROWS = 256
CHUNKS = 4
D = 4096
FF = 1376
V = 4000
GB = ((0, 512), (512, 512), (1024, 352))
VL = ((2752, 1248), (0, 1024), (1376, 1024), (1024, 352), (2400, 352))
VB = ((2752, 512), (3264, 736), (0, 512), (512, 512), (1376, 512), (1888, 512), (1024, 352), (2400, 352))
f32, bf16 = jnp.float32, jnp.bfloat16
MESH = pl.DeviceIdType.MESH

TABLE = {
    (1, 1, 1): [('E1', 0)],
    (1, 1, 3): [('E2', 0)],
    (1, 2, 1): [('E3', 0), ('E1', 1)],
    (1, 3, 0): [('E4', 0), ('E5', 0)],
    (1, 3, 1): [('E2', 1), ('E1', 2)],
    (1, 3, 3): [('E6', 0), ('E3', 1)],
    (1, 3, 4): [],
    (2, 0, 0): [('E7', 0), ('E2', 2)],
    (2, 0, 1): [('E1', 3)],
    (2, 0, 2): [('E4', 1)],
    (2, 1, 0): [('E5', 1), ('E3', 2), ('E6', 1), ('E4', 2), ('E2', 3), ('E7', 1)],
    (2, 1, 1): [('E5', 2)],
    (2, 1, 3): [('E6', 2), ('E3', 3)],
    (2, 2, 0): [('E7', 2)],
    (2, 2, 2): [('E4', 3), ('E5', 3)],
    (2, 3, 0): [('E6', 3), ('E7', 3)],
}

KD, KB1A, KB1B, KB2, KA1, KA2A, KA2B, KA3A, KA3B, KA3C, KA3D = range(11)


def kernel(hid, wg, wu, wd, gain, wv, temp, tgt, out, stats,
           X, PB, DR, B1, B2, W, rsc, ST, SR,
           ssem, rsem, st_s, st_r, xsem, gsem, vsem, credit):
    dp = lax.axis_index('dp')
    y = lax.axis_index('tp2')
    tpi = lax.axis_index('tp')
    x = tpi // 2
    c = tpi % 2
    me = y * 4 + tpi
    f = x + c * (y - x)
    s = y + c * (x - y)
    partner = (dp, y, x * 2 + (1 - c))
    nbr1 = (dp, y + c * (1 - 2 * y), (x + (1 - c) * (1 - 2 * x)) * 2 + c)
    nbr2 = (dp, y + (1 - c) * (1 - 2 * y), (x + c * (1 - 2 * x)) * 2 + c)
    half = c * 128

    def al(v, n):
        return pl.multiple_of(v, n)

    def q(fp, sp):
        return al((2 * fp + sp) * 32, 32)

    def xload(i):
        return pltpu.make_async_copy(hid.at[pl.ds(i * ROWS, ROWS), :], X.at[pl.ds(i * ROWS, ROWS), :], xsem.at[i])

    def gload(b, k):
        src, base = ((wg, 0), (wu, FF))[k]
        r0, n = GB[b]
        return pltpu.make_async_copy(src.at[pl.ds(r0, n), :], W.at[pl.ds(base + r0, n), :], gsem.at[b, k])

    def vload(t):
        r0, n = VL[t]
        return pltpu.make_async_copy(wv.at[pl.ds(r0, n), :], W.at[pl.ds(r0, n), :], vsem.at[t])

    def remote(src, dst, i, k, dev):
        return pltpu.make_async_remote_copy(src_ref=src, dst_ref=dst, send_sem=ssem.at[i, k], recv_sem=rsem.at[i, k],
                                            device_id=dev, device_id_type=MESH)

    def xrows(i, fp, sp, hb):
        return X.at[pl.ds(al(i * ROWS + hb + q(fp, sp), 32), 32), :]

    def prow(i, fp, sp):
        return PB.at[lax.rem(i, 2), pl.ds(al(half + q(fp, sp), 32), 32), :]

    def copy(i, k):
        sl = lax.rem(i, 2)
        if k == KD:
            return remote(PB.at[sl, pl.ds(al(128 - half, 128), 128), :], DR.at[sl], i, k, partner)
        if k == KB1A:
            return remote(prow(i, 1 - f, 1 - s), B1.at[sl, 0], i, k, nbr1)
        if k == KB1B:
            return remote(prow(i, 1 - f, s), B1.at[sl, 1], i, k, nbr1)
        if k == KB2:
            return remote(prow(i, f, 1 - s), B2.at[sl], i, k, nbr2)
        fp, sp = {KA1: (f, s), KA2A: (f, s), KA3A: (f, s), KA2B: (f, 1 - s), KA3B: (f, 1 - s),
                  KA3C: (1 - f, s), KA3D: (1 - f, 1 - s)}[k]
        dev = {KA1: nbr2, KA2A: nbr1, KA2B: nbr1}.get(k, partner)
        r = xrows(i, fp, sp, half)
        return remote(r, r, i, k, dev)

    def e0(i):
        copy(i, KD).start()

    def e1(i):
        copy(i, KD).wait_recv()
        sl = lax.rem(i, 2)
        for sp, k in ((1 - s, KB1A), (s, KB1B)):
            r0 = q(1 - f, sp)

            def add(t, carry):
                pr = pl.ds(al(half + r0 + t * 16, 16), 16)
                dr = pl.ds(al(r0 + t * 16, 16), 16)
                for cb in range(4):
                    cs = slice(cb * 1024, cb * 1024 + 1024)
                    PB[sl, pr, cs] = (PB[sl, pr, cs].astype(f32) + DR[sl, dr, cs].astype(f32)).astype(bf16)
                return carry

            lax.fori_loop(0, 2, add, 0)
            if k == KB1A and i >= 2:
                pl.semaphore_wait(credit.at[1], 1)
            copy(i, k).start()

    def e2(i):
        copy(i, KB1A).wait_recv()
        sl = lax.rem(i, 2)
        r0 = q(f, 1 - s)

        def add(t, carry):
            pr = pl.ds(al(half + r0 + t * 16, 16), 16)
            dr = pl.ds(al(r0 + t * 16, 16), 16)
            br = pl.ds(al(t * 16, 16), 16)
            for cb in range(4):
                cs = slice(cb * 1024, cb * 1024 + 1024)
                PB[sl, pr, cs] = (PB[sl, pr, cs].astype(f32) + DR[sl, dr, cs].astype(f32)
                                  + B1[sl, 0, br, cs].astype(f32)).astype(bf16)
            return carry

        lax.fori_loop(0, 2, add, 0)
        if i >= 2:
            pl.semaphore_wait(credit.at[2], 1)
        copy(i, KB2).start()

    def e3(i):
        copy(i, KB1B).wait_recv()
        copy(i, KB2).wait_recv()
        sl = lax.rem(i, 2)
        r0 = q(f, s)

        def fin(t, carry):
            pr = pl.ds(al(half + r0 + t * 16, 16), 16)
            dr = pl.ds(al(r0 + t * 16, 16), 16)
            br = pl.ds(al(t * 16, 16), 16)
            xr = pl.ds(al(i * ROWS + half + r0 + t * 16, 16), 16)
            acc = jnp.zeros((16, 128), f32)
            for cb in range(16):
                cs = slice(cb * 256, cb * 256 + 256)
                part = (PB[sl, pr, cs].astype(f32) + DR[sl, dr, cs].astype(f32)
                        + B1[sl, 1, br, cs].astype(f32) + B2[sl, br, cs].astype(f32)).astype(bf16)
                r = X[xr, cs].astype(f32) + part.astype(f32)
                rsc[:, cs] = r
                sq = r * r
                acc = acc + sq[:, :128] + sq[:, 128:]
            ms = jnp.sum(acc, axis=1, keepdims=True) * (1.0 / D)
            inv = lax.rsqrt(ms + NORM_EPS)
            for cb in range(16):
                cs = slice(cb * 256, cb * 256 + 256)
                X[xr, cs] = (gain[:, cs] * rsc[:, cs] * inv).astype(bf16)
            return carry

        lax.fori_loop(0, 2, fin, 0)
        copy(i, KA1).start()
        copy(i, KA2A).start()
        copy(i, KA3A).start()
        if i < 2:
            for n, dev in ((0, partner), (1, nbr1), (2, nbr2)):
                pl.semaphore_signal(credit.at[n], inc=1, device_id=dev, device_id_type=MESH)

    def e4(i):
        copy(i, KA1).wait_recv()
        copy(i, KA2B).start()
        copy(i, KA3B).start()

    def e5(i):
        copy(i, KA2A).wait_recv()
        copy(i, KA3C).start()

    def e6(i):
        copy(i, KA2B).wait_recv()
        copy(i, KA3D).start()

    def e7(i):
        for k in (KA3A, KA3B, KA3C, KA3D):
            copy(i, k).wait_recv()

    events = {'E1': e1, 'E2': e2, 'E3': e3, 'E4': e4, 'E5': e5, 'E6': e6, 'E7': e7}

    def progress(phase, i, b):
        for ck in range(CHUNKS):
            todo = TABLE.get((phase, ck, b), [])
            if todo:
                @pl.when(i == ck)
                def _():
                    for name, cc in todo:
                        events[name](cc)

    xload(0).start()
    for b in range(3):
        for k in range(2):
            gload(b, k).start()

    def dott(w, xv):
        return lax.dot_general(w, xv, (((1,), (1,)), ((), ())), preferred_element_type=f32)

    def phase1(wdv, act, dsem):
        def dload(k):
            cs = pl.ds(2048 * k, 2048)
            return pltpu.make_async_copy(wd.at[:, cs], wdv.at[:, cs], dsem.at[k])

        for k in range(2):
            dload(k).start()
        for i in range(1, CHUNKS):
            xload(i).start()

        bar = pltpu.get_barrier_semaphore()
        for d in range(1, 8):
            o = (me + d) % 8
            pl.semaphore_signal(bar, inc=1, device_id=(dp, o // 4, o % 4), device_id_type=MESH)
        pl.semaphore_wait(bar, 7)

        def chunk(i, carry):
            rows = pl.ds(al(i * ROWS, ROWS), ROWS)
            sl = lax.rem(i, 2)
            xload(i).wait()

            def first(fn):
                pl.when(i == 0)(fn)

            def last(fn):
                pl.when(i == CHUNKS - 1)(fn)

            for b, (r0, n) in enumerate(GB):
                @first
                def _():
                    for k in range(2):
                        gload(b, k).wait()

                progress(1, i, b)
                g = dott(W[r0:r0 + n, :], X[rows, :])
                u = dott(W[FF + r0:FF + r0 + n, :], X[rows, :])
                h = g * jax.nn.sigmoid(g) * u
                act[:, r0:r0 + n] = jnp.transpose(h.astype(bf16))

                @last
                def _():
                    for t in ((), (1, 2), (3, 4))[b]:
                        vload(t).start()

            @first
            def _():
                vload(0).start()

            for b in range(2):
                first(lambda: dload(b).wait())
                progress(1, i, 3 + b)
                if b == 0:
                    @pl.when(i >= 2)
                    def _():
                        for k in (KD, KB1A, KB1B, KB2):
                            copy(i - 2, k).wait_send()

                for n in range(8):
                    cs = slice(2048 * b + 256 * n, 2048 * b + 256 * n + 256)
                    PB[sl, :, cs] = jnp.dot(act[...], wdv[:, cs], preferred_element_type=f32).astype(bf16)

            @pl.when(i >= 2)
            def _():
                pl.semaphore_wait(credit.at[0], 1)

            e0(i)
            return carry

        lax.fori_loop(0, CHUNKS, chunk, 0)

    pl.run_scoped(phase1, pltpu.VMEM((FF, D), bf16), pltpu.VMEM((ROWS, FF), bf16), pltpu.SemaphoreType.DMA((2,)))

    def phase2(L, OS, state, IT, TG, LN, osem):
        sub = lax.broadcasted_iota(jnp.int32, (8, ROWS), 0)

        def stats_block(cur, b):
            groups = [r0 + 8 * g for r0, n in VB[2 * b:2 * b + 2] for g in range(n // 8)]
            ms = [L[cur, r:r + 8, :] for r in groups[:4]]
            for k, r in enumerate(groups[4:]):
                ms[k % 4] = jnp.maximum(ms[k % 4], L[cur, r:r + 8, :])
            m_new = jnp.maximum(jnp.maximum(ms[0], ms[1]), jnp.maximum(ms[2], ms[3]))
            zero = jnp.zeros((8, ROWS), f32)
            ss, ws, ts = [zero] * 2, [zero] * 2, [zero] * 2
            if b > 0:
                m_old = state[0]
                m_new = jnp.maximum(m_new, m_old)
                scale = jnp.exp(m_old - m_new)
                ss[0], ws[0], ts[0] = state[1] * scale, state[2] * scale, state[3]
            tg = TG[...]
            for k, r in enumerate(groups):
                l = L[cur, r:r + 8, :]
                e = jnp.exp(l - m_new)
                ss[k % 2] = ss[k % 2] + e
                ws[k % 2] = ws[k % 2] + e * l
                ts[k % 2] = ts[k % 2] + jnp.where(sub == tg - r, l, 0.0)
            state[0] = m_new
            state[1] = ss[0] + ss[1]
            state[2] = ws[0] + ws[1]
            state[3] = ts[0] + ts[1]

        def final_block(old, b):
            for r0, n in VB[2 * b:2 * b + 2]:
                for r in range(r0, r0 + n, 16):
                    OS[r:r + 16, :] = (L[old, r:r + 16, :] - LN[0:1, :]).astype(bf16)

        def stat_copy(i, d):
            o = (me + d) % 8
            return pltpu.make_async_remote_copy(src_ref=ST.at[i], dst_ref=SR.at[i, me], send_sem=st_s.at[i, d],
                                                recv_sem=st_r.at[i, me],
                                                device_id=(dp, o // 4, o % 4), device_id_type=MESH)

        def stat_wait(i, d):
            o = (me + d) % 8
            return pltpu.make_async_remote_copy(src_ref=ST.at[i], dst_ref=SR.at[i, o], send_sem=st_s.at[i, d],
                                                recv_sem=st_r.at[i, o],
                                                device_id=(dp, o // 4, o % 4), device_id_type=MESH)

        def send_stats(i):
            m = state[0]
            mx = jnp.max(m, axis=0, keepdims=True)
            e = jnp.exp(m - mx)
            row = lax.broadcasted_iota(jnp.int32, (8, ROWS), 0)
            pk = jnp.broadcast_to(mx, (8, ROWS))
            for n in (1, 2, 3):
                v = state[n] * e if n < 3 else state[n]
                pk = jnp.where(row == n, jnp.sum(v, axis=0, keepdims=True), pk)
            ST[i] = pk
            SR[i, me] = pk
            for d in range(1, 8):
                stat_copy(i, d).start()

        def recv_stats(i):
            for d in range(1, 8):
                stat_wait(i, d).wait_recv()
            parts = [SR[i, o] for o in range(8)]
            mg = parts[0][0:1, :]
            for p_ in parts[1:]:
                mg = jnp.maximum(mg, p_[0:1, :])
            sg = wgt = tl = jnp.zeros((1, ROWS), f32)
            for p_ in parts:
                e = jnp.exp(p_[0:1, :] - mg)
                sg = sg + p_[1:2, :] * e
                wgt = wgt + p_[2:3, :] * e
                tl = tl + p_[3:4, :]
            lg = mg + jnp.log(sg)
            cs = pl.ds(al(i * ROWS, ROWS), ROWS)
            stats[0:1, cs] = lg
            stats[1:2, cs] = lg - wgt / sg
            stats[2:3, cs] = tl - lg
            LN[...] = jnp.broadcast_to(lg, (8, ROWS))

        def ocopy(i):
            return pltpu.make_async_copy(OS, out.at[:, pl.ds(al(i * ROWS, ROWS), ROWS)], osem)

        def chunk(j, carry):
            rows = pl.ds(al(j * ROWS, ROWS), ROWS)
            cur, old = lax.rem(j, 2), lax.rem(j + 1, 2)
            cs = pl.ds(al(j * ROWS, ROWS), ROWS)
            IT[...] = jnp.broadcast_to(1.0 / temp[:, cs], (8, ROWS))
            tid = tgt[:, cs] - me * V
            TG[...] = jnp.broadcast_to(tid, (8, ROWS))

            def vblock(b):
                for r0, n in VB[2 * b:2 * b + 2]:
                    L[cur, r0:r0 + n, :] = dott(W[r0:r0 + n, :], X[rows, :]) * IT[0:1, :]

            for b in range(4):
                @pl.when(j == 0)
                def _():
                    for t in ((0,), (1,), (2,), (3, 4))[b]:
                        vload(t).wait()

                progress(2, j, b)
                if b == 2:
                    @pl.when(j >= 2)
                    def _():
                        ocopy(j - 2).wait()

                    @pl.when(j >= 1)
                    def _():
                        recv_stats(j - 1)
                if b >= 1:
                    stats_block(cur, b - 1)
                vblock(b)
                if b >= 2:
                    @pl.when(j >= 1)
                    def _():
                        final_block(old, 2 * b - 4)
                        final_block(old, 2 * b - 3)
            stats_block(cur, 3)
            send_stats(j)

            @pl.when(j >= 1)
            def _():
                ocopy(j - 1).start()

            return carry

        lax.fori_loop(0, CHUNKS, chunk, 0)
        ocopy(CHUNKS - 2).wait()
        recv_stats(CHUNKS - 1)
        for b in range(4):
            final_block((CHUNKS - 1) % 2, b)
        ocopy(CHUNKS - 1).start()
        for i in range(CHUNKS):
            for k in range(11):
                if k > KB2 or i >= 2:
                    copy(i, k).wait_send()
            for d in range(1, 8):
                stat_copy(i, d).wait_send()
        ocopy(CHUNKS - 1).wait()

    pl.run_scoped(phase2, pltpu.VMEM((2, V, ROWS), f32), pltpu.VMEM((V, ROWS), bf16),
                  pltpu.VMEM((4, 8, ROWS), f32), pltpu.VMEM((8, ROWS), f32), pltpu.VMEM((8, ROWS), jnp.int32),
                  pltpu.VMEM((8, ROWS), f32), pltpu.SemaphoreType.DMA)


def solution(mesh):
    model_axes = ('tp2', 'tp')

    def local_step(hidden, w_gate, w_up, w_down, norm_gain, w_vocab, temperature, target_ids):
        n = hidden.shape[0]
        anyspec = pl.BlockSpec(memory_space=pl.ANY)
        vspec = pl.BlockSpec(memory_space=pltpu.VMEM)
        logprobs, stats = pl.pallas_call(
            kernel,
            out_shape=(jax.ShapeDtypeStruct((V, n), bf16), jax.ShapeDtypeStruct((8, n), f32)),
            in_specs=[anyspec, anyspec, anyspec, anyspec, vspec, anyspec, vspec, vspec],
            out_specs=(anyspec, vspec),
            scratch_shapes=[
                pltpu.VMEM((n, D), bf16),
                pltpu.VMEM((2, ROWS, D), bf16),
                pltpu.VMEM((2, ROWS // 2, D), bf16),
                pltpu.VMEM((2, 2, ROWS // 8, D), bf16),
                pltpu.VMEM((2, ROWS // 8, D), bf16),
                pltpu.VMEM((V, D), bf16),
                pltpu.VMEM((16, D), f32),
                pltpu.VMEM((CHUNKS, 8, ROWS), f32),
                pltpu.VMEM((CHUNKS, 8, 8, ROWS), f32),
                pltpu.SemaphoreType.DMA((CHUNKS, 11)),
                pltpu.SemaphoreType.DMA((CHUNKS, 11)),
                pltpu.SemaphoreType.DMA((CHUNKS, 8)),
                pltpu.SemaphoreType.DMA((CHUNKS, 8)),
                pltpu.SemaphoreType.DMA((CHUNKS,)),
                pltpu.SemaphoreType.DMA((3, 2)),
                pltpu.SemaphoreType.DMA((5,)),
                pltpu.SemaphoreType.REGULAR((3,)),
            ],
            compiler_params=pltpu.CompilerParams(collective_id=0, has_side_effects=True, vmem_limit_bytes=67043328),
        )(hidden, w_gate.T, w_up.T, w_down, norm_gain.reshape(1, D), w_vocab.T,
          temperature.reshape(1, n), target_ids.reshape(1, n))
        return stats[0], stats[1], stats[2], logprobs.T

    return jax.shard_map(
        local_step, mesh=mesh,
        in_specs=(P('dp', None), P(None, model_axes), P(None, model_axes), P(model_axes, None),
                  P(None), P(None, model_axes), P('dp'), P('dp')),
        out_specs=(P('dp'), P('dp'), P('dp'), P('dp', model_axes)),
        check_vma=False)
```

```python
import functools

import jax
import jax.numpy as jnp
from jax import lax
from jax.experimental import pallas as pl
from jax.experimental.pallas import tpu as pltpu
from jax.sharding import PartitionSpec as P

NORM_EPS = 1e-6
ROWS = 256
CHUNKS = 4
D = 4096
FF = 1376
V = 4000
GB = ((0, 256), (256, 256), (512, 512), (1024, 352))
VL = ((2752, 1248), (0, 1024), (1376, 1024), (1024, 352), (2400, 352))
VB = (((2752, 624), (3376, 624)), ((0, 512), (512, 512)), ((1376, 512), (1888, 512)), ((1024, 352), (2400, 352)))
VN = (1248, 1024, 1024, 704)
VR = (((2752, 0, 1248),), ((0, 0, 1024),), ((1376, 0, 1024),), ((1024, 0, 352), (2400, 352, 352)))
f32, bf16 = jnp.float32, jnp.bfloat16
MESH = pl.DeviceIdType.MESH

B1B_LATE = False
TABLE = {
    (1, 1, 0): [('E1a', 0)],
    (1, 1, 2): [('E1b', 0)],
    (2, 1, 0): [('E2a', 0)],
    (2, 1, 1): [('E2b', 0), ('E1a', 1)],
    (1, 2, 0): [('E3', 0)],
    (1, 2, 2): [('E1b', 1)],
    (1, 2, 3): [('E2a', 1)],
    (2, 2, 1): [('E4', 0)],
    (1, 3, 1): [('E1a', 2), ('E2b', 1)],
    (1, 3, 3): [('E3', 1), ('E5', 0)],
    (2, 3, 1): [('E2a', 2), ('E6', 0), ('E1b', 2), ('E7', 0)],
    (3, 0, 1): [('E4', 1)],
    (3, 0, 2): [('E2b', 2), ('E5', 1), ('E1a', 3)],
    (3, 0, 3): [('E1b', 3), ('E3', 2)],
    (3, 1, 0): [('E6', 1), ('E7', 1)],
    (3, 1, 1): [('E2a', 3)],
    (3, 1, 2): [('E4', 2), ('E2b', 3)],
    (3, 2, 0): [('E5', 2), ('E3', 3), ('E6', 2), ('E7', 2)],
    (3, 2, 2): [('E4', 3), ('E5', 3)],
    (3, 3, 0): [('E6', 3), ('E7', 3)],
}

KD, KB1A, KB1B, KB2, KA1, KA2A, KA2B, KA3A, KA3B, KA3C, KA3D = 0, 2, 4, 6, 8, 9, 10, 11, 12, 13, 14
NK = 15


def kernel(hid, wg, wu, wd, gain, wv, temp, tgt, out, last_l, stats,
           X, PB, DR, B1, B2, W, rsc, ST, SR,
           ssem, rsem, st_s, st_r, xsem, gsem, vsem, credit):
    dp = lax.axis_index('dp')
    y = lax.axis_index('tp2')
    tpi = lax.axis_index('tp')
    x = tpi // 2
    c = tpi % 2
    me = y * 4 + tpi
    f = x + c * (y - x)
    s = y + c * (x - y)
    partner = (dp, y, x * 2 + (1 - c))
    nbr1 = (dp, y + c * (1 - 2 * y), (x + (1 - c) * (1 - 2 * x)) * 2 + c)
    nbr2 = (dp, y + (1 - c) * (1 - 2 * y), (x + c * (1 - 2 * x)) * 2 + c)
    half = c * 128

    def al(v, n):
        return pl.multiple_of(v, n)

    def q(fp, sp):
        return al((2 * fp + sp) * 32, 32)

    def xload(i):
        return pltpu.make_async_copy(hid.at[pl.ds(i * ROWS, ROWS), :], X.at[pl.ds(i * ROWS, ROWS), :], xsem.at[i])

    def gload(b, k):
        src, base = ((wg, 0), (wu, FF))[k]
        r0, n = GB[b]
        return pltpu.make_async_copy(src.at[pl.ds(r0, n), :], W.at[pl.ds(base + r0, n), :], gsem.at[b, k])

    def vload(t):
        r0, n = VL[t]
        return pltpu.make_async_copy(wv.at[pl.ds(r0, n), :], W.at[pl.ds(r0, n), :], vsem.at[t])

    def remote(src, dst, i, k, dev):
        return pltpu.make_async_remote_copy(src_ref=src, dst_ref=dst, send_sem=ssem.at[i, k], recv_sem=rsem.at[i, k],
                                            device_id=dev, device_id_type=MESH)

    def xrows(i, fp, sp, hb):
        return X.at[pl.ds(al(i * ROWS + hb + q(fp, sp), 32), 32), :]

    def prow(i, fp, sp, cs):
        return PB.at[lax.rem(i, 2), pl.ds(al(half + q(fp, sp), 32), 32), cs]

    def copy(i, k):
        sl = lax.rem(i, 2)
        if k < KA1:
            kind = k - k % 2
            cs = pl.ds(2048 * (k % 2), 2048)
            if kind == KD:
                return remote(PB.at[sl, pl.ds(al(128 - half, 128), 128), cs], DR.at[sl, :, cs], i, k, partner)
            if kind == KB1A:
                return remote(prow(i, 1 - f, 1 - s, cs), B1.at[sl, 0, :, cs], i, k, nbr1)
            if kind == KB1B:
                return remote(prow(i, 1 - f, s, cs), B1.at[sl, 1, :, cs], i, k, nbr1)
            return remote(prow(i, f, 1 - s, cs), B2.at[sl, :, cs], i, k, nbr2)
        fp, sp = {KA1: (f, s), KA2A: (f, s), KA3A: (f, s), KA2B: (f, 1 - s), KA3B: (f, 1 - s),
                  KA3C: (1 - f, s), KA3D: (1 - f, 1 - s)}[k]
        dev = {KA1: nbr2, KA2A: nbr1, KA2B: nbr1}.get(k, partner)
        r = xrows(i, fp, sp, half)
        return remote(r, r, i, k, dev)

    def e1(i, h):
        copy(i, KD + h).wait_recv()
        sl = lax.rem(i, 2)
        for sp, k in ((1 - s, KB1A), (s, KB1B)):
            r0 = q(1 - f, sp)

            def add(t, carry):
                pr = pl.ds(al(half + r0 + t * 16, 16), 16)
                dr = pl.ds(al(r0 + t * 16, 16), 16)
                for cb in range(2):
                    cs = slice(2048 * h + cb * 1024, 2048 * h + cb * 1024 + 1024)
                    PB[sl, pr, cs] = (PB[sl, pr, cs].astype(f32) + DR[sl, dr, cs].astype(f32)).astype(bf16)
                return carry

            lax.fori_loop(0, 2, add, 0)
            if k == KB1A and i >= 2 and h == 0:
                pl.semaphore_wait(credit.at[1], 1)
            if k == KB1A or not B1B_LATE:
                copy(i, k + h).start()

    def e2(i, h):
        copy(i, KB1A + h).wait_recv()
        sl = lax.rem(i, 2)
        r0 = q(f, 1 - s)

        def add(t, carry):
            pr = pl.ds(al(half + r0 + t * 16, 16), 16)
            dr = pl.ds(al(r0 + t * 16, 16), 16)
            br = pl.ds(al(t * 16, 16), 16)
            for cb in range(2):
                cs = slice(2048 * h + cb * 1024, 2048 * h + cb * 1024 + 1024)
                PB[sl, pr, cs] = (PB[sl, pr, cs].astype(f32) + DR[sl, dr, cs].astype(f32)
                                  + B1[sl, 0, br, cs].astype(f32)).astype(bf16)
            return carry

        lax.fori_loop(0, 2, add, 0)
        if i >= 2 and h == 0:
            pl.semaphore_wait(credit.at[2], 1)
        copy(i, KB2 + h).start()
        if B1B_LATE:
            copy(i, KB1B + h).start()

    def e3(i):
        for h in range(2):
            copy(i, KB1B + h).wait_recv()
            copy(i, KB2 + h).wait_recv()
        sl = lax.rem(i, 2)
        r0 = q(f, s)

        def fin(t, carry):
            pr = pl.ds(al(half + r0 + t * 16, 16), 16)
            dr = pl.ds(al(r0 + t * 16, 16), 16)
            br = pl.ds(al(t * 16, 16), 16)
            xr = pl.ds(al(i * ROWS + half + r0 + t * 16, 16), 16)
            acc = jnp.zeros((16, 128), f32)
            for cb in range(16):
                cs = slice(cb * 256, cb * 256 + 256)
                part = (PB[sl, pr, cs].astype(f32) + DR[sl, dr, cs].astype(f32)
                        + B1[sl, 1, br, cs].astype(f32) + B2[sl, br, cs].astype(f32)).astype(bf16)
                r = X[xr, cs].astype(f32) + part.astype(f32)
                rsc[:, cs] = r
                sq = r * r
                acc = acc + sq[:, :128] + sq[:, 128:]
            ms = jnp.sum(acc, axis=1, keepdims=True) * (1.0 / D)
            inv = lax.rsqrt(ms + NORM_EPS)
            for cb in range(16):
                cs = slice(cb * 256, cb * 256 + 256)
                X[xr, cs] = (gain[:, cs] * rsc[:, cs] * inv).astype(bf16)
            return carry

        lax.fori_loop(0, 2, fin, 0)
        copy(i, KA1).start()
        copy(i, KA2A).start()
        copy(i, KA3A).start()
        if i < 2:
            for n, dev in ((0, partner), (1, nbr1), (2, nbr2)):
                pl.semaphore_signal(credit.at[n], inc=1, device_id=dev, device_id_type=MESH)

    def e4(i):
        copy(i, KA1).wait_recv()
        copy(i, KA2B).start()
        copy(i, KA3B).start()

    def e5(i):
        copy(i, KA2A).wait_recv()
        copy(i, KA3C).start()

    def e6(i):
        copy(i, KA2B).wait_recv()
        copy(i, KA3D).start()

    def e7(i):
        for k in (KA3A, KA3B, KA3C, KA3D):
            copy(i, k).wait_recv()

    events = {'E3': e3, 'E4': e4, 'E5': e5, 'E6': e6, 'E7': e7}
    for h_, n_ in ((0, 'a'), (1, 'b')):
        events['E1' + n_] = functools.partial(e1, h=h_)
        events['E2' + n_] = functools.partial(e2, h=h_)

    def progress(phase, i, b):
        for ck in range(CHUNKS):
            todo = TABLE.get((phase, ck, b), [])
            if todo:
                @pl.when(i == ck)
                def _():
                    for name, cc in todo:
                        events[name](cc)

    xload(0).start()
    for b in range(4):
        for k in range(2):
            gload(b, k).start()

    def dott(w, xv):
        return lax.dot_general(w, xv, (((1,), (1,)), ((), ())), preferred_element_type=f32)

    def phase1(wdv, act, dsem):
        def dload(k):
            cs = pl.ds(2048 * k, 2048)
            return pltpu.make_async_copy(wd.at[:, cs], wdv.at[:, cs], dsem.at[k])

        for k in range(2):
            dload(k).start()
        for i in range(1, CHUNKS):
            xload(i).start()

        bar = pltpu.get_barrier_semaphore()
        for d in range(1, 8):
            o = (me + d) % 8
            pl.semaphore_signal(bar, inc=1, device_id=(dp, o // 4, o % 4), device_id_type=MESH)
        pl.semaphore_wait(bar, 7)

        def chunk(i, carry):
            rows = pl.ds(al(i * ROWS, ROWS), ROWS)
            sl = lax.rem(i, 2)
            xload(i).wait()

            def first(fn):
                pl.when(i == 0)(fn)

            def last(fn):
                pl.when(i == CHUNKS - 1)(fn)

            for b, (r0, n) in enumerate(GB):
                @first
                def _():
                    for k in range(2):
                        gload(b, k).wait()

                progress(1, i, b)
                g = dott(W[r0:r0 + n, :], X[rows, :])
                u = dott(W[FF + r0:FF + r0 + n, :], X[rows, :])
                h = g * jax.nn.sigmoid(g) * u
                act[:, r0:r0 + n] = jnp.transpose(h.astype(bf16))

                @last
                def _():
                    for t in ((), (), (1, 2), (3, 4))[b]:
                        vload(t).start()

            @first
            def _():
                vload(0).start()

            for b in range(2):
                first(lambda: dload(b).wait())
                progress(2, i, b)
                if b == 0:
                    @pl.when(i >= 2)
                    def _():
                        for k in range(KA1):
                            copy(i - 2, k).wait_send()
                        pl.semaphore_wait(credit.at[0], 1)

                for n in range(8):
                    cs = slice(2048 * b + 256 * n, 2048 * b + 256 * n + 256)
                    PB[sl, :, cs] = jnp.dot(act[...], wdv[:, cs], preferred_element_type=f32).astype(bf16)

                copy(i, KD + b).start()

            return carry

        lax.fori_loop(0, CHUNKS, chunk, 0)

    pl.run_scoped(phase1, pltpu.VMEM((FF, D), bf16), pltpu.VMEM((ROWS, FF), bf16), pltpu.SemaphoreType.DMA((2,)))

    def phase2(L0, L1, L2, L3, OS, state, IT, TG, LN, osem, lsem):
        L = (L0, L1, L2, L3)
        sub = lax.broadcasted_iota(jnp.int32, (8, ROWS), 0)

        def stats_block(cur, b):
            groups = [(lo + k, v + k) for v, lo, n in VR[b] for k in range(0, n, 8)]
            ms = [L[b][cur, r:r + 8, :] for r, _ in groups[:4]]
            for k, (r, _) in enumerate(groups[4:]):
                ms[k % 4] = jnp.maximum(ms[k % 4], L[b][cur, r:r + 8, :])
            m_new = jnp.maximum(jnp.maximum(ms[0], ms[1]), jnp.maximum(ms[2], ms[3]))
            zero = jnp.zeros((8, ROWS), f32)
            ss, ws, ts = [zero] * 2, [zero] * 2, [zero] * 2
            if b > 0:
                m_old = state[0]
                m_new = jnp.maximum(m_new, m_old)
                scale = jnp.exp(m_old - m_new)
                ss[0], ws[0], ts[0] = state[1] * scale, state[2] * scale, state[3]
            tg = TG[...]
            for k, (r, v) in enumerate(groups):
                l = L[b][cur, r:r + 8, :]
                e = jnp.exp(l - m_new)
                ss[k % 2] = ss[k % 2] + e
                ws[k % 2] = ws[k % 2] + e * l
                ts[k % 2] = ts[k % 2] + jnp.where(sub == tg - v, l, 0.0)
            state[0] = m_new
            state[1] = ss[0] + ss[1]
            state[2] = ws[0] + ws[1]
            state[3] = ts[0] + ts[1]

        def final_block(old, b):
            for v, lo, n in VR[b]:
                for k in range(0, n, 16):
                    OS[v + k:v + k + 16, :] = (L[b][old, lo + k:lo + k + 16, :] - LN[0:1, :]).astype(bf16)

        def ocopies(i, blocks):
            return [pltpu.make_async_copy(OS.at[pl.ds(v, n), :], out.at[pl.ds(v, n), pl.ds(al(i * ROWS, ROWS), ROWS)],
                                          osem.at[b, k]) for b in blocks for k, (v, lo, n) in enumerate(VR[b])]

        def lcopies(b):
            return [pltpu.make_async_copy(L[b].at[(CHUNKS - 1) % 2, pl.ds(lo, n), :], last_l.at[pl.ds(v, n), :], lsem.at[b, k])
                    for k, (v, lo, n) in enumerate(VR[b])]

        def stat_copy(i, d):
            o = (me + d) % 8
            return pltpu.make_async_remote_copy(src_ref=ST.at[i], dst_ref=SR.at[i, me], send_sem=st_s.at[i, d],
                                                recv_sem=st_r.at[i, me],
                                                device_id=(dp, o // 4, o % 4), device_id_type=MESH)

        def stat_wait(i, d):
            o = (me + d) % 8
            return pltpu.make_async_remote_copy(src_ref=ST.at[i], dst_ref=SR.at[i, o], send_sem=st_s.at[i, d],
                                                recv_sem=st_r.at[i, o],
                                                device_id=(dp, o // 4, o % 4), device_id_type=MESH)

        def send_stats(i):
            m = state[0]
            mx = jnp.max(m, axis=0, keepdims=True)
            e = jnp.exp(m - mx)
            row = lax.broadcasted_iota(jnp.int32, (8, ROWS), 0)
            pk = jnp.broadcast_to(mx, (8, ROWS))
            for n in (1, 2, 3):
                v = state[n] * e if n < 3 else state[n]
                pk = jnp.where(row == n, jnp.sum(v, axis=0, keepdims=True), pk)
            ST[i] = pk
            SR[i, me] = pk
            for d in range(1, 8):
                stat_copy(i, d).start()

        def recv_stats(i):
            for d in range(1, 8):
                stat_wait(i, d).wait_recv()
            parts = [SR[i, o] for o in range(8)]
            mg = parts[0][0:1, :]
            for p_ in parts[1:]:
                mg = jnp.maximum(mg, p_[0:1, :])
            sg = wgt = tl = jnp.zeros((1, ROWS), f32)
            for p_ in parts:
                e = jnp.exp(p_[0:1, :] - mg)
                sg = sg + p_[1:2, :] * e
                wgt = wgt + p_[2:3, :] * e
                tl = tl + p_[3:4, :]
            lg = mg + jnp.log(sg)
            cs = pl.ds(al(i * ROWS, ROWS), ROWS)
            stats[0:1, cs] = lg
            stats[1:2, cs] = lg - wgt / sg
            stats[2:3, cs] = tl - lg
            LN[...] = jnp.broadcast_to(lg, (8, ROWS))

        def chunk(j, carry):
            rows = pl.ds(al(j * ROWS, ROWS), ROWS)
            cur, old = lax.rem(j, 2), lax.rem(j + 1, 2)
            cs = pl.ds(al(j * ROWS, ROWS), ROWS)
            IT[...] = jnp.broadcast_to(1.0 / temp[:, cs], (8, ROWS))
            tid = tgt[:, cs] - me * V
            TG[...] = jnp.broadcast_to(tid, (8, ROWS))

            def vblock(b):
                lo = 0
                for r0, n in VB[b]:
                    L[b][cur, lo:lo + n, :] = dott(W[r0:r0 + n, :], X[rows, :]) * IT[0:1, :]
                    lo += n

            for b in range(4):
                @pl.when(j == 0)
                def _():
                    for t in ((0,), (1,), (2,), (3, 4))[b]:
                        vload(t).wait()

                progress(3, j, b)
                if b == 2:
                    @pl.when(j >= 2)
                    def _():
                        for cp in ocopies(j - 2, range(4)):
                            cp.wait()

                    @pl.when(j >= 1)
                    def _():
                        recv_stats(j - 1)

                vblock(b)
                if b >= 1:
                    stats_block(cur, b - 1)
                if b >= 2:
                    done = (2 * b - 4, 2 * b - 3)
                    for d in done:
                        final_block(old, d)

                    @pl.when(j >= 1)
                    def _():
                        for cp in ocopies(j - 1, done):
                            cp.start()

                @pl.when(j == CHUNKS - 1)
                def _():
                    for cp in lcopies(b):
                        cp.start()

            stats_block(cur, 3)
            send_stats(j)
            return carry

        lax.fori_loop(0, CHUNKS, chunk, 0)
        for i in range(CHUNKS):
            for k in range(NK):
                if k >= KA1 or i >= 2:
                    copy(i, k).wait_send()
        for cp in ocopies(CHUNKS - 2, range(4)):
            cp.wait()
        for b in range(4):
            for cp in lcopies(b):
                cp.wait()
        recv_stats(CHUNKS - 1)
        for i in range(CHUNKS):
            for d in range(1, 8):
                stat_copy(i, d).wait_send()

    pl.run_scoped(phase2, *[pltpu.VMEM((2, n, ROWS), f32) for n in VN], pltpu.VMEM((V, ROWS), bf16),
                  pltpu.VMEM((4, 8, ROWS), f32), pltpu.VMEM((8, ROWS), f32), pltpu.VMEM((8, ROWS), jnp.int32),
                  pltpu.VMEM((8, ROWS), f32), pltpu.SemaphoreType.DMA((4, 2)), pltpu.SemaphoreType.DMA((4, 2)))


def finish(lp_ref, l_ref, st_ref, out_ref, s0, s1, s2):
    n = lp_ref.shape[1]
    out_ref[:, :n] = lp_ref[...]
    out_ref[:, n:] = (l_ref[...] - st_ref[0:1, n:]).astype(bf16)
    s0[...] = st_ref[0:1, :]
    s1[...] = st_ref[1:2, :]
    s2[...] = st_ref[2:3, :]


def solution(mesh):
    model_axes = ('tp2', 'tp')

    def local_step(hidden, w_gate, w_up, w_down, norm_gain, w_vocab, temperature, target_ids):
        n = hidden.shape[0]
        anyspec = pl.BlockSpec(memory_space=pl.ANY)
        vspec = pl.BlockSpec(memory_space=pltpu.VMEM)
        early, last_l, stats = pl.pallas_call(
            kernel,
            out_shape=(jax.ShapeDtypeStruct((V, n), bf16), jax.ShapeDtypeStruct((V, ROWS), f32),
                       jax.ShapeDtypeStruct((8, n), f32)),
            in_specs=[anyspec, anyspec, anyspec, anyspec, vspec, anyspec, vspec, vspec],
            out_specs=(anyspec, anyspec, vspec),
            scratch_shapes=[
                pltpu.VMEM((n, D), bf16),
                pltpu.VMEM((2, ROWS, D), bf16),
                pltpu.VMEM((2, ROWS // 2, D), bf16),
                pltpu.VMEM((2, 2, ROWS // 8, D), bf16),
                pltpu.VMEM((2, ROWS // 8, D), bf16),
                pltpu.VMEM((V, D), bf16),
                pltpu.VMEM((16, D), f32),
                pltpu.VMEM((CHUNKS, 8, ROWS), f32),
                pltpu.VMEM((CHUNKS, 8, 8, ROWS), f32),
                pltpu.SemaphoreType.DMA((CHUNKS, NK)),
                pltpu.SemaphoreType.DMA((CHUNKS, NK)),
                pltpu.SemaphoreType.DMA((CHUNKS, 8)),
                pltpu.SemaphoreType.DMA((CHUNKS, 8)),
                pltpu.SemaphoreType.DMA((CHUNKS,)),
                pltpu.SemaphoreType.DMA((4, 2)),
                pltpu.SemaphoreType.DMA((5,)),
                pltpu.SemaphoreType.REGULAR((3,)),
            ],
            compiler_params=pltpu.CompilerParams(collective_id=0, has_side_effects=True, vmem_limit_bytes=67043328),
        )(hidden, w_gate.T, w_up.T, w_down, norm_gain.reshape(1, D), w_vocab.T,
          temperature.reshape(1, n), target_ids.reshape(1, n))
        row = pl.BlockSpec((1, n), lambda i: (0, 0))
        logprobs, s0, s1, s2 = pl.pallas_call(
            finish,
            grid=(10,),
            out_shape=(jax.ShapeDtypeStruct((V, n), bf16),) + (jax.ShapeDtypeStruct((1, n), f32),) * 3,
            in_specs=[pl.BlockSpec((V // 10, n - ROWS), lambda i: (i, 0)), pl.BlockSpec((V // 10, ROWS), lambda i: (i, 0)),
                      pl.BlockSpec((8, n), lambda i: (0, 0))],
            out_specs=(pl.BlockSpec((V // 10, n), lambda i: (i, 0)), row, row, row),
        )(early, last_l, stats)
        return s0.reshape(n), s1.reshape(n), s2.reshape(n), logprobs.T

    return jax.shard_map(
        local_step, mesh=mesh,
        in_specs=(P('dp', None), P(None, model_axes), P(None, model_axes), P(model_axes, None),
                  P(None), P(None, model_axes), P('dp'), P('dp')),
        out_specs=(P('dp'), P('dp'), P('dp'), P('dp', model_axes)),
        check_vma=False)
```

```python
import functools

import jax
import jax.numpy as jnp
from jax import lax
from jax.experimental import pallas as pl
from jax.experimental.pallas import tpu as pltpu
from jax.sharding import PartitionSpec as P

NORM_EPS = 1e-6
ROWS = 256
CHUNKS = 4
D = 4096
PIECE = 400
FF = 1376
V = 4000
GB = ((0, 256), (256, 256), (512, 512), (1024, 352))
VL = ((2752, 1248), (0, 1024), (1376, 1024), (1024, 352), (2400, 352))
VB = (((2752, 624), (3376, 624)), ((0, 512), (512, 512)), ((1376, 512), (1888, 512)), ((1024, 352), (2400, 352)))
VN = (1248, 1024, 1024, 704)
VR = (((2752, 0, 1248),), ((0, 0, 1024),), ((1376, 0, 1024),), ((1024, 0, 352), (2400, 352, 352)))
f32, bf16 = jnp.float32, jnp.bfloat16
MESH = pl.DeviceIdType.MESH

B1B_LATE = False
TABLE = {
    (1, 1, 0): [('E1a', 0)],
    (1, 1, 2): [('E1b', 0)],
    (2, 1, 0): [('E2a', 0)],
    (2, 1, 1): [('E2b', 0), ('E1a', 1)],
    (1, 2, 0): [('E3', 0)],
    (1, 2, 2): [('E1b', 1)],
    (1, 2, 3): [('E2a', 1)],
    (2, 2, 1): [('E4', 0)],
    (1, 3, 1): [('E1a', 2), ('E2b', 1)],
    (1, 3, 3): [('E3', 1), ('E5', 0)],
    (2, 3, 1): [('E2a', 2), ('E6', 0), ('E1b', 2), ('E7', 0)],
    (3, 0, 1): [('E4', 1)],
    (3, 0, 2): [('E2b', 2), ('E5', 1), ('E1a', 3)],
    (3, 0, 3): [('E1b', 3), ('E3', 2)],
    (3, 1, 0): [('E6', 1), ('E7', 1)],
    (3, 1, 1): [('E2a', 3)],
    (3, 1, 2): [('E4', 2), ('E2b', 3)],
    (3, 2, 0): [('E5', 2), ('E3', 3), ('E6', 2), ('E7', 2)],
    (3, 2, 2): [('E4', 3), ('E5', 3)],
    (3, 3, 0): [('E6', 3), ('E7', 3)],
}

KD, KB1A, KB1B, KB2, KA1, KA2A, KA2B, KA3A, KA3B, KA3C, KA3D = 0, 2, 4, 6, 8, 9, 10, 11, 12, 13, 14
NK = 15


def kernel(hid, wg, wu, wd, gain, wv, temp, tgt, out, last_l, stats,
           X, PB, DR, B1, B2, W, rsc, ST, SR,
           ssem, rsem, st_s, st_r, xsem, gsem, vsem, credit):
    dp = lax.axis_index('dp')
    y = lax.axis_index('tp2')
    tpi = lax.axis_index('tp')
    x = tpi // 2
    c = tpi % 2
    me = y * 4 + tpi
    f = x + c * (y - x)
    s = y + c * (x - y)
    partner = (dp, y, x * 2 + (1 - c))
    nbr1 = (dp, y + c * (1 - 2 * y), (x + (1 - c) * (1 - 2 * x)) * 2 + c)
    nbr2 = (dp, y + (1 - c) * (1 - 2 * y), (x + c * (1 - 2 * x)) * 2 + c)
    half = c * 128

    def al(v, n):
        return pl.multiple_of(v, n)

    def q(fp, sp):
        return al((2 * fp + sp) * 32, 32)

    def xload(i):
        return pltpu.make_async_copy(hid.at[pl.ds(i * ROWS, ROWS), :], X.at[pl.ds(i * ROWS, ROWS), :], xsem.at[i])

    def gload(b, k):
        src, base = ((wg, 0), (wu, FF))[k]
        r0, n = GB[b]
        return pltpu.make_async_copy(src.at[pl.ds(r0, n), :], W.at[pl.ds(base + r0, n), :], gsem.at[b, k])

    def vload(t):
        r0, n = VL[t]
        return pltpu.make_async_copy(wv.at[pl.ds(r0, n), :], W.at[pl.ds(r0, n), :], vsem.at[t])

    def remote(src, dst, i, k, dev):
        return pltpu.make_async_remote_copy(src_ref=src, dst_ref=dst, send_sem=ssem.at[i, k], recv_sem=rsem.at[i, k],
                                            device_id=dev, device_id_type=MESH)

    def xrows(i, fp, sp, hb):
        return X.at[pl.ds(al(i * ROWS + hb + q(fp, sp), 32), 32), :]

    def prow(i, fp, sp, cs):
        return PB.at[lax.rem(i, 2), pl.ds(al(half + q(fp, sp), 32), 32), cs]

    def copy(i, k):
        sl = lax.rem(i, 2)
        if k < KA1:
            kind = k - k % 2
            cs = pl.ds(2048 * (k % 2), 2048)
            if kind == KD:
                return remote(PB.at[sl, pl.ds(al(128 - half, 128), 128), cs], DR.at[sl, :, cs], i, k, partner)
            if kind == KB1A:
                return remote(prow(i, 1 - f, 1 - s, cs), B1.at[sl, 0, :, cs], i, k, nbr1)
            if kind == KB1B:
                return remote(prow(i, 1 - f, s, cs), B1.at[sl, 1, :, cs], i, k, nbr1)
            return remote(prow(i, f, 1 - s, cs), B2.at[sl, :, cs], i, k, nbr2)
        fp, sp = {KA1: (f, s), KA2A: (f, s), KA3A: (f, s), KA2B: (f, 1 - s), KA3B: (f, 1 - s),
                  KA3C: (1 - f, s), KA3D: (1 - f, 1 - s)}[k]
        dev = {KA1: nbr2, KA2A: nbr1, KA2B: nbr1}.get(k, partner)
        r = xrows(i, fp, sp, half)
        return remote(r, r, i, k, dev)

    def e1(i, h):
        copy(i, KD + h).wait_recv()
        sl = lax.rem(i, 2)
        for sp, k in ((1 - s, KB1A), (s, KB1B)):
            r0 = q(1 - f, sp)

            def add(t, carry):
                pr = pl.ds(al(half + r0 + t * 16, 16), 16)
                dr = pl.ds(al(r0 + t * 16, 16), 16)
                for cb in range(2):
                    cs = slice(2048 * h + cb * 1024, 2048 * h + cb * 1024 + 1024)
                    PB[sl, pr, cs] = (PB[sl, pr, cs].astype(f32) + DR[sl, dr, cs].astype(f32)).astype(bf16)
                return carry

            lax.fori_loop(0, 2, add, 0)
            if k == KB1A and i >= 2 and h == 0:
                pl.semaphore_wait(credit.at[1], 1)
            if k == KB1A or not B1B_LATE:
                copy(i, k + h).start()

    def e2(i, h):
        copy(i, KB1A + h).wait_recv()
        sl = lax.rem(i, 2)
        r0 = q(f, 1 - s)

        def add(t, carry):
            pr = pl.ds(al(half + r0 + t * 16, 16), 16)
            dr = pl.ds(al(r0 + t * 16, 16), 16)
            br = pl.ds(al(t * 16, 16), 16)
            for cb in range(2):
                cs = slice(2048 * h + cb * 1024, 2048 * h + cb * 1024 + 1024)
                PB[sl, pr, cs] = (PB[sl, pr, cs].astype(f32) + DR[sl, dr, cs].astype(f32)
                                  + B1[sl, 0, br, cs].astype(f32)).astype(bf16)
            return carry

        lax.fori_loop(0, 2, add, 0)
        if i >= 2 and h == 0:
            pl.semaphore_wait(credit.at[2], 1)
        copy(i, KB2 + h).start()
        if B1B_LATE:
            copy(i, KB1B + h).start()

    def e3(i):
        for h in range(2):
            copy(i, KB1B + h).wait_recv()
            copy(i, KB2 + h).wait_recv()
        sl = lax.rem(i, 2)
        r0 = q(f, s)

        def fin(t, carry):
            pr = pl.ds(al(half + r0 + t * 16, 16), 16)
            dr = pl.ds(al(r0 + t * 16, 16), 16)
            br = pl.ds(al(t * 16, 16), 16)
            xr = pl.ds(al(i * ROWS + half + r0 + t * 16, 16), 16)
            acc = jnp.zeros((16, 128), f32)
            for cb in range(16):
                cs = slice(cb * 256, cb * 256 + 256)
                part = (PB[sl, pr, cs].astype(f32) + DR[sl, dr, cs].astype(f32)
                        + B1[sl, 1, br, cs].astype(f32) + B2[sl, br, cs].astype(f32)).astype(bf16)
                r = X[xr, cs].astype(f32) + part.astype(f32)
                rsc[:, cs] = r
                sq = r * r
                acc = acc + sq[:, :128] + sq[:, 128:]
            ms = jnp.sum(acc, axis=1, keepdims=True) * (1.0 / D)
            inv = lax.rsqrt(ms + NORM_EPS)
            for cb in range(16):
                cs = slice(cb * 256, cb * 256 + 256)
                X[xr, cs] = (gain[:, cs] * rsc[:, cs] * inv).astype(bf16)
            return carry

        lax.fori_loop(0, 2, fin, 0)
        copy(i, KA1).start()
        copy(i, KA2A).start()
        copy(i, KA3A).start()
        if i < 2:
            for n, dev in ((0, partner), (1, nbr1), (2, nbr2)):
                pl.semaphore_signal(credit.at[n], inc=1, device_id=dev, device_id_type=MESH)

    def e4(i):
        copy(i, KA1).wait_recv()
        copy(i, KA2B).start()
        copy(i, KA3B).start()

    def e5(i):
        copy(i, KA2A).wait_recv()
        copy(i, KA3C).start()

    def e6(i):
        copy(i, KA2B).wait_recv()
        copy(i, KA3D).start()

    def e7(i):
        for k in (KA3A, KA3B, KA3C, KA3D):
            copy(i, k).wait_recv()

    events = {'E3': e3, 'E4': e4, 'E5': e5, 'E6': e6, 'E7': e7}
    for h_, n_ in ((0, 'a'), (1, 'b')):
        events['E1' + n_] = functools.partial(e1, h=h_)
        events['E2' + n_] = functools.partial(e2, h=h_)

    def progress(phase, i, b):
        for ck in range(CHUNKS):
            todo = TABLE.get((phase, ck, b), [])
            if todo:
                @pl.when(i == ck)
                def _():
                    for name, cc in todo:
                        with jax.named_scope(f'{name}_{cc}'):
                            events[name](cc)

    xload(0).start()
    for b in range(4):
        for k in range(2):
            gload(b, k).start()

    def dott(w, xv):
        return lax.dot_general(w, xv, (((1,), (1,)), ((), ())), preferred_element_type=f32)

    def phase1(wdv, act, dsem):
        def dload(k):
            cs = pl.ds(2048 * k, 2048)
            return pltpu.make_async_copy(wd.at[:, cs], wdv.at[:, cs], dsem.at[k])

        for k in range(2):
            dload(k).start()
        for i in range(1, CHUNKS):
            xload(i).start()

        bar = pltpu.get_barrier_semaphore()
        for d in range(1, 8):
            o = (me + d) % 8
            pl.semaphore_signal(bar, inc=1, device_id=(dp, o // 4, o % 4), device_id_type=MESH)
        pl.semaphore_wait(bar, 7)

        def chunk(i, carry):
            rows = pl.ds(al(i * ROWS, ROWS), ROWS)
            sl = lax.rem(i, 2)
            xload(i).wait()

            def first(fn):
                pl.when(i == 0)(fn)

            def last(fn):
                pl.when(i == CHUNKS - 1)(fn)

            for b, (r0, n) in enumerate(GB):
                @first
                def _():
                    for k in range(2):
                        gload(b, k).wait()

                progress(1, i, b)
                with jax.named_scope(f'G{b}'):
                    g = dott(W[r0:r0 + n, :], X[rows, :])
                    u = dott(W[FF + r0:FF + r0 + n, :], X[rows, :])
                    h = g * jax.nn.sigmoid(g) * u
                    act[:, r0:r0 + n] = jnp.transpose(h.astype(bf16))

                @last
                def _():
                    for t in ((), (), (1, 2), (3, 4))[b]:
                        vload(t).start()

            @first
            def _():
                vload(0).start()

            for b in range(2):
                first(lambda: dload(b).wait())
                progress(2, i, b)
                if b == 0:
                    @pl.when(i >= 2)
                    def _():
                        for k in range(KA1):
                            copy(i - 2, k).wait_send()
                        pl.semaphore_wait(credit.at[0], 1)

                with jax.named_scope(f'D{b}'):
                    for n in range(8):
                        cs = slice(2048 * b + 256 * n, 2048 * b + 256 * n + 256)
                        PB[sl, :, cs] = jnp.dot(act[...], wdv[:, cs], preferred_element_type=f32).astype(bf16)

                copy(i, KD + b).start()

            return carry

        lax.fori_loop(0, CHUNKS, chunk, 0)

    pl.run_scoped(phase1, pltpu.VMEM((FF, D), bf16), pltpu.VMEM((ROWS, FF), bf16), pltpu.SemaphoreType.DMA((2,)))

    def phase2(L0, L1, L2, L3, OS, state, IT, TG, LN, osem, lsem):
        L = (L0, L1, L2, L3)
        sub = lax.broadcasted_iota(jnp.int32, (8, ROWS), 0)

        def stats_block(cur, b):
            groups = [(lo + k, v + k) for v, lo, n in VR[b] for k in range(0, n, 8)]
            ms = [L[b][cur, r:r + 8, :] for r, _ in groups[:4]]
            for k, (r, _) in enumerate(groups[4:]):
                ms[k % 4] = jnp.maximum(ms[k % 4], L[b][cur, r:r + 8, :])
            m_new = jnp.maximum(jnp.maximum(ms[0], ms[1]), jnp.maximum(ms[2], ms[3]))
            zero = jnp.zeros((8, ROWS), f32)
            ss, ws, ts = [zero] * 2, [zero] * 2, [zero] * 2
            if b > 0:
                m_old = state[0]
                m_new = jnp.maximum(m_new, m_old)
                scale = jnp.exp(m_old - m_new)
                ss[0], ws[0], ts[0] = state[1] * scale, state[2] * scale, state[3]
            tg = TG[...]
            for k, (r, v) in enumerate(groups):
                l = L[b][cur, r:r + 8, :]
                e = jnp.exp(l - m_new)
                ss[k % 2] = ss[k % 2] + e
                ws[k % 2] = ws[k % 2] + e * l
                ts[k % 2] = ts[k % 2] + jnp.where(sub == tg - v, l, 0.0)
            state[0] = m_new
            state[1] = ss[0] + ss[1]
            state[2] = ws[0] + ws[1]
            state[3] = ts[0] + ts[1]

        def final_block(old, b):
            for v, lo, n in VR[b]:
                for k in range(0, n, 16):
                    OS[v + k:v + k + 16, :] = (L[b][old, lo + k:lo + k + 16, :] - LN[0:1, :]).astype(bf16)

        def ocopies(i, blocks):
            return [pltpu.make_async_copy(OS.at[pl.ds(v, n), :], out.at[pl.ds(v, n), pl.ds(al(i * ROWS, ROWS), ROWS)],
                                          osem.at[b, k]) for b in blocks for k, (v, lo, n) in enumerate(VR[b])]

        def lcopies(b):
            return [pltpu.make_async_copy(L[b].at[(CHUNKS - 1) % 2, pl.ds(lo, n), :], last_l.at[pl.ds(v, n), :], lsem.at[b, k])
                    for k, (v, lo, n) in enumerate(VR[b])]

        def stat_copy(i, d):
            o = (me + d) % 8
            return pltpu.make_async_remote_copy(src_ref=ST.at[i], dst_ref=SR.at[i, me], send_sem=st_s.at[i, d],
                                                recv_sem=st_r.at[i, me],
                                                device_id=(dp, o // 4, o % 4), device_id_type=MESH)

        def stat_wait(i, d):
            o = (me + d) % 8
            return pltpu.make_async_remote_copy(src_ref=ST.at[i], dst_ref=SR.at[i, o], send_sem=st_s.at[i, d],
                                                recv_sem=st_r.at[i, o],
                                                device_id=(dp, o // 4, o % 4), device_id_type=MESH)

        def send_stats(i):
            m = state[0]
            mx = jnp.max(m, axis=0, keepdims=True)
            e = jnp.exp(m - mx)
            row = lax.broadcasted_iota(jnp.int32, (8, ROWS), 0)
            pk = jnp.broadcast_to(mx, (8, ROWS))
            for n in (1, 2, 3):
                v = state[n] * e if n < 3 else state[n]
                pk = jnp.where(row == n, jnp.sum(v, axis=0, keepdims=True), pk)
            ST[i] = pk
            SR[i, me] = pk
            for d in range(1, 8):
                stat_copy(i, d).start()

        def recv_stats(i):
            for d in range(1, 8):
                stat_wait(i, d).wait_recv()
            parts = [SR[i, o] for o in range(8)]
            mg = parts[0][0:1, :]
            for p_ in parts[1:]:
                mg = jnp.maximum(mg, p_[0:1, :])
            sg = wgt = tl = jnp.zeros((1, ROWS), f32)
            for p_ in parts:
                e = jnp.exp(p_[0:1, :] - mg)
                sg = sg + p_[1:2, :] * e
                wgt = wgt + p_[2:3, :] * e
                tl = tl + p_[3:4, :]
            lg = mg + jnp.log(sg)
            cs = pl.ds(al(i * ROWS, ROWS), ROWS)
            stats[0:1, cs] = lg
            stats[1:2, cs] = lg - wgt / sg
            stats[2:3, cs] = tl - lg
            LN[...] = jnp.broadcast_to(lg, (8, ROWS))

        def chunk(j, carry):
            rows = pl.ds(al(j * ROWS, ROWS), ROWS)
            cur, old = lax.rem(j, 2), lax.rem(j + 1, 2)
            cs = pl.ds(al(j * ROWS, ROWS), ROWS)
            IT[...] = jnp.broadcast_to(1.0 / temp[:, cs], (8, ROWS))
            tid = tgt[:, cs] - me * V
            TG[...] = jnp.broadcast_to(tid, (8, ROWS))

            def vblock(b):
                lo = 0
                for r0, n in VB[b]:
                    L[b][cur, lo:lo + n, :] = dott(W[r0:r0 + n, :], X[rows, :]) * IT[0:1, :]
                    lo += n

            for b in range(4):
                @pl.when(j == 0)
                def _():
                    for t in ((0,), (1,), (2,), (3, 4))[b]:
                        vload(t).wait()

                progress(3, j, b)
                if b == 2:
                    @pl.when(j >= 2)
                    def _():
                        for cp in ocopies(j - 2, range(4)):
                            cp.wait()

                    @pl.when(j >= 1)
                    def _():
                        with jax.named_scope('RST'):
                            recv_stats(j - 1)

                with jax.named_scope(f'V{b}'):
                    vblock(b)
                    if b >= 1:
                        stats_block(cur, b - 1)
                if b >= 2:
                    done = (2 * b - 4, 2 * b - 3)
                    for d in done:
                        final_block(old, d)

                    @pl.when(j >= 1)
                    def _():
                        for cp in ocopies(j - 1, done):
                            cp.start()

                @pl.when(j == CHUNKS - 1)
                def _():
                    for cp in lcopies(b):
                        cp.start()

            with jax.named_scope('STL'):
                stats_block(cur, 3)
                send_stats(j)
            return carry

        lax.fori_loop(0, CHUNKS, chunk, 0)
        for i in range(CHUNKS):
            for k in range(NK):
                if k >= KA1 or i >= 2:
                    copy(i, k).wait_send()
        for cp in ocopies(CHUNKS - 2, range(4)):
            cp.wait()
        for b in range(4):
            for cp in lcopies(b):
                cp.wait()
        with jax.named_scope('RSTL'):
            recv_stats(CHUNKS - 1)
        for i in range(CHUNKS):
            for d in range(1, 8):
                stat_copy(i, d).wait_send()

    pl.run_scoped(phase2, *[pltpu.VMEM((2, n, ROWS), f32) for n in VN], pltpu.VMEM((V, ROWS), bf16),
                  pltpu.VMEM((4, 8, ROWS), f32), pltpu.VMEM((8, ROWS), f32), pltpu.VMEM((8, ROWS), jnp.int32),
                  pltpu.VMEM((8, ROWS), f32), pltpu.SemaphoreType.DMA((4, 2)), pltpu.SemaphoreType.DMA((4, 2)))


def finish(lp, l, st_ref, out, s0, s1, s2, lpv, lv, ov, isem, jsem, osem, psem):
    n = lpv.shape[1]
    pieces = range(V // PIECE)

    def rows(k):
        return pl.ds(k * PIECE, PIECE)

    early = [pltpu.make_async_copy(lp.at[rows(k), pl.ds(0, n)], lpv.at[rows(k), :], isem.at[k]) for k in pieces]
    late = [pltpu.make_async_copy(l.at[rows(k), :], lv.at[rows(k), :], jsem.at[k]) for k in pieces]
    put = [pltpu.make_async_copy(lpv.at[rows(k), :], out.at[rows(k), pl.ds(0, n)], osem.at[k]) for k in pieces]
    end = [pltpu.make_async_copy(ov.at[rows(k), :], out.at[rows(k), pl.ds(n, ROWS)], psem.at[k]) for k in pieces]
    for k in pieces:
        early[k].start()
        late[k].start()
    s0[...] = st_ref[0:1, :]
    s1[...] = st_ref[1:2, :]
    s2[...] = st_ref[2:3, :]
    for k in pieces:
        early[k].wait()
        put[k].start()
        late[k].wait()
        r = k * PIECE
        ov[r:r + PIECE, :] = (lv[r:r + PIECE, :] - st_ref[0:1, n:]).astype(bf16)
        end[k].start()
    for k in pieces:
        put[k].wait()
        end[k].wait()


def solution(mesh):
    model_axes = ('tp2', 'tp')

    def local_step(hidden, w_gate, w_up, w_down, norm_gain, w_vocab, temperature, target_ids):
        n = hidden.shape[0]
        anyspec = pl.BlockSpec(memory_space=pl.ANY)
        vspec = pl.BlockSpec(memory_space=pltpu.VMEM)
        early, last_l, stats = pl.pallas_call(
            kernel,
            out_shape=(jax.ShapeDtypeStruct((V, n), bf16), jax.ShapeDtypeStruct((V, ROWS), f32),
                       jax.ShapeDtypeStruct((8, n), f32)),
            in_specs=[anyspec, anyspec, anyspec, anyspec, vspec, anyspec, vspec, vspec],
            out_specs=(anyspec, anyspec, vspec),
            scratch_shapes=[
                pltpu.VMEM((n, D), bf16),
                pltpu.VMEM((2, ROWS, D), bf16),
                pltpu.VMEM((2, ROWS // 2, D), bf16),
                pltpu.VMEM((2, 2, ROWS // 8, D), bf16),
                pltpu.VMEM((2, ROWS // 8, D), bf16),
                pltpu.VMEM((V, D), bf16),
                pltpu.VMEM((16, D), f32),
                pltpu.VMEM((CHUNKS, 8, ROWS), f32),
                pltpu.VMEM((CHUNKS, 8, 8, ROWS), f32),
                pltpu.SemaphoreType.DMA((CHUNKS, NK)),
                pltpu.SemaphoreType.DMA((CHUNKS, NK)),
                pltpu.SemaphoreType.DMA((CHUNKS, 8)),
                pltpu.SemaphoreType.DMA((CHUNKS, 8)),
                pltpu.SemaphoreType.DMA((CHUNKS,)),
                pltpu.SemaphoreType.DMA((4, 2)),
                pltpu.SemaphoreType.DMA((5,)),
                pltpu.SemaphoreType.REGULAR((3,)),
            ],
            compiler_params=pltpu.CompilerParams(collective_id=0, has_side_effects=True, vmem_limit_bytes=67043328),
        )(hidden, w_gate.T, w_up.T, w_down, norm_gain.reshape(1, D), w_vocab.T,
          temperature.reshape(1, n), target_ids.reshape(1, n))
        dma = pltpu.SemaphoreType.DMA((V // PIECE,))
        logprobs, s0, s1, s2 = pl.pallas_call(
            finish,
            out_shape=(jax.ShapeDtypeStruct((V, n), bf16),) + (jax.ShapeDtypeStruct((1, n), f32),) * 3,
            in_specs=[anyspec, anyspec, vspec],
            out_specs=(anyspec, vspec, vspec, vspec),
            scratch_shapes=[pltpu.VMEM((V, n - ROWS), bf16), pltpu.VMEM((V, ROWS), f32), pltpu.VMEM((V, ROWS), bf16),
                            dma, dma, dma, dma],
            compiler_params=pltpu.CompilerParams(vmem_limit_bytes=67043328),
        )(early, last_l, stats)
        return s0.reshape(n), s1.reshape(n), s2.reshape(n), logprobs.T

    return jax.shard_map(
        local_step, mesh=mesh,
        in_specs=(P('dp', None), P(None, model_axes), P(None, model_axes), P(model_axes, None),
                  P(None), P(None, model_axes), P('dp'), P('dp')),
        out_specs=(P('dp'), P('dp'), P('dp'), P('dp', model_axes)),
        check_vma=False)
```

```python
import functools

import jax
import jax.numpy as jnp
from jax import lax
from jax.experimental import pallas as pl
from jax.experimental.pallas import tpu as pltpu
from jax.sharding import PartitionSpec as P

NORM_EPS = 1e-6
ROWS = 256
CHUNKS = 4
D = 4096
PIECE = 400
FF = 1376
V = 4000
GB = ((0, 256), (256, 256), (512, 512), (1024, 352))
VL = ((2752, 1248), (0, 1024), (1376, 1024), (1024, 352), (2400, 352))
VB = (((2752, 624), (3376, 624)), ((0, 512), (512, 512)), ((1376, 512), (1888, 512)), ((1024, 352), (2400, 352)))
VN = (1248, 1024, 1024, 704)
VR = (((2752, 0, 1248),), ((0, 0, 1024),), ((1376, 0, 1024),), ((1024, 0, 352), (2400, 352, 352)))
f32, bf16 = jnp.float32, jnp.bfloat16
MESH = pl.DeviceIdType.MESH

B1B_LATE = False
TABLE = {
    (1, 1, 0): [('E1a', 0)],
    (1, 1, 2): [('E1b', 0)],
    (1, 1, 3): [('E2a', 0)],
    (2, 1, 1): [('E2b', 0), ('E1a', 1)],
    (1, 2, 0): [('E3', 0)],
    (1, 2, 2): [('E1b', 1)],
    (2, 2, 0): [('E2a', 1), ('E4', 0)],
    (2, 2, 1): [('E2b', 1), ('E1a', 2)],
    (1, 3, 1): [('E3', 1)],
    (2, 3, 0): [('E1b', 2), ('E5', 0)],
    (2, 3, 1): [('E2a', 2), ('E6', 0)],
    (3, 0, 0): [('E7', 0), ('E4', 1)],
    (3, 0, 1): [('E1a', 3)],
    (3, 0, 2): [('E1b', 3), ('E2b', 2), ('E5', 1)],
    (3, 0, 3): [('E6', 1), ('E3', 2)],
    (3, 1, 0): [('E7', 1)],
    (3, 1, 1): [('E2a', 3), ('E2b', 3)],
    (3, 1, 2): [('E4', 2)],
    (3, 1, 3): [('E3', 3)],
    (3, 2, 0): [('E5', 2), ('E6', 2), ('E7', 2)],
    (3, 2, 1): [('E4', 3)],
    (3, 2, 2): [('E5', 3)],
    (3, 2, 3): [('E6', 3)],
    (3, 3, 0): [('E7', 3)],
}

KD, KB1A, KB1B, KB2, KA1, KA2A, KA2B, KA3A, KA3B, KA3C, KA3D = 0, 2, 4, 6, 8, 9, 10, 11, 12, 13, 14
NK = 15


def kernel(hid, wg, wu, wd, gain, wv, temp, tgt, out, last_l, stats,
           X, PB, DR, B1, B2, W, rsc, ST, SR,
           ssem, rsem, st_s, st_r, xsem, gsem, vsem, credit):
    dp = lax.axis_index('dp')
    y = lax.axis_index('tp2')
    tpi = lax.axis_index('tp')
    x = tpi // 2
    c = tpi % 2
    me = y * 4 + tpi
    f = x + c * (y - x)
    s = y + c * (x - y)
    partner = (dp, y, x * 2 + (1 - c))
    nbr1 = (dp, y + c * (1 - 2 * y), (x + (1 - c) * (1 - 2 * x)) * 2 + c)
    nbr2 = (dp, y + (1 - c) * (1 - 2 * y), (x + c * (1 - 2 * x)) * 2 + c)
    half = c * 128

    def al(v, n):
        return pl.multiple_of(v, n)

    def q(fp, sp):
        return al((2 * fp + sp) * 32, 32)

    def xload(i):
        return pltpu.make_async_copy(hid.at[pl.ds(i * ROWS, ROWS), :], X.at[pl.ds(i * ROWS, ROWS), :], xsem.at[i])

    def gload(b, k):
        src, base = ((wg, 0), (wu, FF))[k]
        r0, n = GB[b]
        return pltpu.make_async_copy(src.at[pl.ds(r0, n), :], W.at[pl.ds(base + r0, n), :], gsem.at[b, k])

    def vload(t):
        r0, n = VL[t]
        return pltpu.make_async_copy(wv.at[pl.ds(r0, n), :], W.at[pl.ds(r0, n), :], vsem.at[t])

    def remote(src, dst, i, k, dev):
        return pltpu.make_async_remote_copy(src_ref=src, dst_ref=dst, send_sem=ssem.at[i, k], recv_sem=rsem.at[i, k],
                                            device_id=dev, device_id_type=MESH)

    def xrows(i, fp, sp, hb):
        return X.at[pl.ds(al(i * ROWS + hb + q(fp, sp), 32), 32), :]

    def prow(i, fp, sp, cs):
        return PB.at[lax.rem(i, 2), pl.ds(al(half + q(fp, sp), 32), 32), cs]

    def copy(i, k):
        sl = lax.rem(i, 2)
        if k < KA1:
            kind = k - k % 2
            cs = pl.ds(2048 * (k % 2), 2048)
            if kind == KD:
                return remote(PB.at[sl, pl.ds(al(128 - half, 128), 128), cs], DR.at[sl, :, cs], i, k, partner)
            if kind == KB1A:
                return remote(prow(i, 1 - f, 1 - s, cs), B1.at[sl, 0, :, cs], i, k, nbr1)
            if kind == KB1B:
                return remote(prow(i, 1 - f, s, cs), B1.at[sl, 1, :, cs], i, k, nbr1)
            return remote(prow(i, f, 1 - s, cs), B2.at[sl, :, cs], i, k, nbr2)
        fp, sp = {KA1: (f, s), KA2A: (f, s), KA3A: (f, s), KA2B: (f, 1 - s), KA3B: (f, 1 - s),
                  KA3C: (1 - f, s), KA3D: (1 - f, 1 - s)}[k]
        dev = {KA1: nbr2, KA2A: nbr1, KA2B: nbr1}.get(k, partner)
        r = xrows(i, fp, sp, half)
        return remote(r, r, i, k, dev)

    def e1(i, h):
        copy(i, KD + h).wait_recv()
        sl = lax.rem(i, 2)
        for sp, k in ((1 - s, KB1A), (s, KB1B)):
            r0 = q(1 - f, sp)

            def add(t, carry):
                pr = pl.ds(al(half + r0 + t * 16, 16), 16)
                dr = pl.ds(al(r0 + t * 16, 16), 16)
                for cb in range(2):
                    cs = slice(2048 * h + cb * 1024, 2048 * h + cb * 1024 + 1024)
                    PB[sl, pr, cs] = (PB[sl, pr, cs].astype(f32) + DR[sl, dr, cs].astype(f32)).astype(bf16)
                return carry

            lax.fori_loop(0, 2, add, 0)
            if k == KB1A and i >= 2 and h == 0:
                pl.semaphore_wait(credit.at[1], 1)
            if k == KB1A or not B1B_LATE:
                copy(i, k + h).start()

    def e2(i, h):
        copy(i, KB1A + h).wait_recv()
        sl = lax.rem(i, 2)
        r0 = q(f, 1 - s)

        def add(t, carry):
            pr = pl.ds(al(half + r0 + t * 16, 16), 16)
            dr = pl.ds(al(r0 + t * 16, 16), 16)
            br = pl.ds(al(t * 16, 16), 16)
            for cb in range(2):
                cs = slice(2048 * h + cb * 1024, 2048 * h + cb * 1024 + 1024)
                PB[sl, pr, cs] = (PB[sl, pr, cs].astype(f32) + DR[sl, dr, cs].astype(f32)
                                  + B1[sl, 0, br, cs].astype(f32)).astype(bf16)
            return carry

        lax.fori_loop(0, 2, add, 0)
        if i >= 2 and h == 0:
            pl.semaphore_wait(credit.at[2], 1)
        copy(i, KB2 + h).start()
        if B1B_LATE:
            copy(i, KB1B + h).start()

    def e3(i):
        for h in range(2):
            copy(i, KB1B + h).wait_recv()
            copy(i, KB2 + h).wait_recv()
        sl = lax.rem(i, 2)
        r0 = q(f, s)

        def fin(t, carry):
            pr = pl.ds(al(half + r0 + t * 16, 16), 16)
            dr = pl.ds(al(r0 + t * 16, 16), 16)
            br = pl.ds(al(t * 16, 16), 16)
            xr = pl.ds(al(i * ROWS + half + r0 + t * 16, 16), 16)
            acc = jnp.zeros((16, 128), f32)
            for cb in range(16):
                cs = slice(cb * 256, cb * 256 + 256)
                part = (PB[sl, pr, cs].astype(f32) + DR[sl, dr, cs].astype(f32)
                        + B1[sl, 1, br, cs].astype(f32) + B2[sl, br, cs].astype(f32)).astype(bf16)
                r = X[xr, cs].astype(f32) + part.astype(f32)
                rsc[:, cs] = r
                sq = r * r
                acc = acc + sq[:, :128] + sq[:, 128:]
            ms = jnp.sum(acc, axis=1, keepdims=True) * (1.0 / D)
            inv = lax.rsqrt(ms + NORM_EPS)
            for cb in range(16):
                cs = slice(cb * 256, cb * 256 + 256)
                X[xr, cs] = (gain[:, cs] * rsc[:, cs] * inv).astype(bf16)
            return carry

        lax.fori_loop(0, 2, fin, 0)
        copy(i, KA1).start()
        copy(i, KA2A).start()
        copy(i, KA3A).start()
        if i < 2:
            for n, dev in ((0, partner), (1, nbr1), (2, nbr2)):
                pl.semaphore_signal(credit.at[n], inc=1, device_id=dev, device_id_type=MESH)

    def e4(i):
        copy(i, KA1).wait_recv()
        copy(i, KA2B).start()
        copy(i, KA3B).start()

    def e5(i):
        copy(i, KA2A).wait_recv()
        copy(i, KA3C).start()

    def e6(i):
        copy(i, KA2B).wait_recv()
        copy(i, KA3D).start()

    def e7(i):
        for k in (KA3A, KA3B, KA3C, KA3D):
            copy(i, k).wait_recv()

    events = {'E3': e3, 'E4': e4, 'E5': e5, 'E6': e6, 'E7': e7}
    for h_, n_ in ((0, 'a'), (1, 'b')):
        events['E1' + n_] = functools.partial(e1, h=h_)
        events['E2' + n_] = functools.partial(e2, h=h_)

    def progress(phase, i, b):
        for ck in range(CHUNKS):
            todo = TABLE.get((phase, ck, b), [])
            if todo:
                @pl.when(i == ck)
                def _():
                    for name, cc in todo:
                        with jax.named_scope(f'{name}_{cc}'):
                            events[name](cc)

    xload(0).start()
    for b in range(2):
        for k in range(2):
            gload(b, k).start()

    def dott(w, xv):
        return lax.dot_general(w, xv, (((1,), (1,)), ((), ())), preferred_element_type=f32)

    def phase1(wdv, act, dsem):
        def dload(k):
            cs = pl.ds(2048 * k, 2048)
            return pltpu.make_async_copy(wd.at[:, cs], wdv.at[:, cs], dsem.at[k])


        bar = pltpu.get_barrier_semaphore()
        for d in range(1, 8):
            o = (me + d) % 8
            pl.semaphore_signal(bar, inc=1, device_id=(dp, o // 4, o % 4), device_id_type=MESH)
        with jax.named_scope('BAR'):
            pl.semaphore_wait(bar, 7)
        for k in range(2):
            gload(2, k).start()

        def chunk(i, carry):
            rows = pl.ds(al(i * ROWS, ROWS), ROWS)
            sl = lax.rem(i, 2)
            xload(i).wait()

            def first(fn):
                pl.when(i == 0)(fn)

            def last(fn):
                pl.when(i == CHUNKS - 1)(fn)

            for b, (r0, n) in enumerate(GB):
                @first
                def _():
                    for k in range(2):
                        gload(b, k).wait()
                    for cp in ((gload(3, 0), gload(3, 1)), (dload(0), dload(1)), (xload(1), xload(2), xload(3)), ())[b]:
                        cp.start()

                progress(1, i, b)
                with jax.named_scope(f'G{b}'):
                    g = dott(W[r0:r0 + n, :], X[rows, :])
                    u = dott(W[FF + r0:FF + r0 + n, :], X[rows, :])
                    h = g * jax.nn.sigmoid(g) * u
                    act[:, r0:r0 + n] = jnp.transpose(h.astype(bf16))

                @last
                def _():
                    for t in ((), (), (1, 2), (3, 4))[b]:
                        vload(t).start()

            @first
            def _():
                vload(0).start()

            for b in range(2):
                first(lambda: dload(b).wait())
                progress(2, i, b)
                if b == 0:
                    @pl.when(i >= 2)
                    def _():
                        for k in range(KA1):
                            copy(i - 2, k).wait_send()
                        pl.semaphore_wait(credit.at[0], 1)

                with jax.named_scope(f'D{b}'):
                    for n in range(8):
                        cs = slice(2048 * b + 256 * n, 2048 * b + 256 * n + 256)
                        PB[sl, :, cs] = jnp.dot(act[...], wdv[:, cs], preferred_element_type=f32).astype(bf16)

                copy(i, KD + b).start()

            return carry

        lax.fori_loop(0, CHUNKS, chunk, 0)

    pl.run_scoped(phase1, pltpu.VMEM((FF, D), bf16), pltpu.VMEM((ROWS, FF), bf16), pltpu.SemaphoreType.DMA((2,)))

    def phase2(L0, L1, L2, L3, OS, state, IT, TG, LN, osem, lsem):
        L = (L0, L1, L2, L3)
        sub = lax.broadcasted_iota(jnp.int32, (8, ROWS), 0)

        def stats_block(cur, b):
            groups = [(lo + k, v + k) for v, lo, n in VR[b] for k in range(0, n, 8)]
            ms = [L[b][cur, r:r + 8, :] for r, _ in groups[:4]]
            for k, (r, _) in enumerate(groups[4:]):
                ms[k % 4] = jnp.maximum(ms[k % 4], L[b][cur, r:r + 8, :])
            m_new = jnp.maximum(jnp.maximum(ms[0], ms[1]), jnp.maximum(ms[2], ms[3]))
            zero = jnp.zeros((8, ROWS), f32)
            ss, ws, ts = [zero] * 2, [zero] * 2, [zero] * 2
            if b > 0:
                m_old = state[0]
                m_new = jnp.maximum(m_new, m_old)
                scale = jnp.exp(m_old - m_new)
                ss[0], ws[0], ts[0] = state[1] * scale, state[2] * scale, state[3]
            tg = TG[...]
            for k, (r, v) in enumerate(groups):
                l = L[b][cur, r:r + 8, :]
                e = jnp.exp(l - m_new)
                ss[k % 2] = ss[k % 2] + e
                ws[k % 2] = ws[k % 2] + e * l
                ts[k % 2] = ts[k % 2] + jnp.where(sub == tg - v, l, 0.0)
            state[0] = m_new
            state[1] = ss[0] + ss[1]
            state[2] = ws[0] + ws[1]
            state[3] = ts[0] + ts[1]

        def final_block(old, b):
            for v, lo, n in VR[b]:
                for k in range(0, n, 16):
                    OS[v + k:v + k + 16, :] = (L[b][old, lo + k:lo + k + 16, :] - LN[0:1, :]).astype(bf16)

        def ocopies(i, blocks):
            return [pltpu.make_async_copy(OS.at[pl.ds(v, n), :], out.at[pl.ds(v, n), pl.ds(al(i * ROWS, ROWS), ROWS)],
                                          osem.at[b, k]) for b in blocks for k, (v, lo, n) in enumerate(VR[b])]

        def lcopies(b):
            return [pltpu.make_async_copy(L[b].at[(CHUNKS - 1) % 2, pl.ds(lo, n), :], last_l.at[pl.ds(v, n), :], lsem.at[b, k])
                    for k, (v, lo, n) in enumerate(VR[b])]

        def stat_copy(i, d):
            o = (me + d) % 8
            return pltpu.make_async_remote_copy(src_ref=ST.at[i], dst_ref=SR.at[i, me], send_sem=st_s.at[i, d],
                                                recv_sem=st_r.at[i, me],
                                                device_id=(dp, o // 4, o % 4), device_id_type=MESH)

        def stat_wait(i, d):
            o = (me + d) % 8
            return pltpu.make_async_remote_copy(src_ref=ST.at[i], dst_ref=SR.at[i, o], send_sem=st_s.at[i, d],
                                                recv_sem=st_r.at[i, o],
                                                device_id=(dp, o // 4, o % 4), device_id_type=MESH)

        def send_stats(i):
            m = state[0]
            mx = jnp.max(m, axis=0, keepdims=True)
            e = jnp.exp(m - mx)
            row = lax.broadcasted_iota(jnp.int32, (8, ROWS), 0)
            pk = jnp.broadcast_to(mx, (8, ROWS))
            for n in (1, 2, 3):
                v = state[n] * e if n < 3 else state[n]
                pk = jnp.where(row == n, jnp.sum(v, axis=0, keepdims=True), pk)
            ST[i] = pk
            SR[i, me] = pk
            for d in range(1, 8):
                stat_copy(i, d).start()

        def recv_stats(i):
            for d in range(1, 8):
                stat_wait(i, d).wait_recv()
            parts = [SR[i, o] for o in range(8)]
            mg = parts[0][0:1, :]
            for p_ in parts[1:]:
                mg = jnp.maximum(mg, p_[0:1, :])
            sg = wgt = tl = jnp.zeros((1, ROWS), f32)
            for p_ in parts:
                e = jnp.exp(p_[0:1, :] - mg)
                sg = sg + p_[1:2, :] * e
                wgt = wgt + p_[2:3, :] * e
                tl = tl + p_[3:4, :]
            lg = mg + jnp.log(sg)
            cs = pl.ds(al(i * ROWS, ROWS), ROWS)
            stats[0:1, cs] = lg
            stats[1:2, cs] = lg - wgt / sg
            stats[2:3, cs] = tl - lg
            LN[...] = jnp.broadcast_to(lg, (8, ROWS))

        def chunk(j, carry):
            rows = pl.ds(al(j * ROWS, ROWS), ROWS)
            cur, old = lax.rem(j, 2), lax.rem(j + 1, 2)
            cs = pl.ds(al(j * ROWS, ROWS), ROWS)
            IT[...] = jnp.broadcast_to(1.0 / temp[:, cs], (8, ROWS))
            tid = tgt[:, cs] - me * V
            TG[...] = jnp.broadcast_to(tid, (8, ROWS))

            def vblock(b):
                lo = 0
                for r0, n in VB[b]:
                    L[b][cur, lo:lo + n, :] = dott(W[r0:r0 + n, :], X[rows, :]) * IT[0:1, :]
                    lo += n

            for b in range(4):
                @pl.when(j == 0)
                def _():
                    for t in ((0,), (1,), (2,), (3, 4))[b]:
                        vload(t).wait()

                progress(3, j, b)
                if b == 3:
                    @pl.when(j >= 2)
                    def _():
                        for cp in ocopies(j - 2, range(4)):
                            cp.wait()

                    @pl.when(j >= 1)
                    def _():
                        with jax.named_scope('RST'):
                            recv_stats(j - 1)

                with jax.named_scope(f'V{b}'):
                    vblock(b)
                    if b >= 1:
                        stats_block(cur, b - 1)
                if b == 3:
                    done = range(4)
                    for d in done:
                        final_block(old, d)

                    @pl.when(j >= 1)
                    def _():
                        for cp in ocopies(j - 1, done):
                            cp.start()

                @pl.when(j == CHUNKS - 1)
                def _():
                    for cp in lcopies(b):
                        cp.start()

            with jax.named_scope('STL'):
                stats_block(cur, 3)
                send_stats(j)
            return carry

        lax.fori_loop(0, CHUNKS, chunk, 0)
        for i in range(CHUNKS):
            for k in range(NK):
                if k >= KA1 or i >= 2:
                    copy(i, k).wait_send()
        for cp in ocopies(CHUNKS - 2, range(4)):
            cp.wait()
        for b in range(4):
            for cp in lcopies(b):
                cp.wait()
        with jax.named_scope('RSTL'):
            recv_stats(CHUNKS - 1)
        for i in range(CHUNKS):
            for d in range(1, 8):
                stat_copy(i, d).wait_send()

    pl.run_scoped(phase2, *[pltpu.VMEM((2, n, ROWS), f32) for n in VN], pltpu.VMEM((V, ROWS), bf16),
                  pltpu.VMEM((4, 8, ROWS), f32), pltpu.VMEM((8, ROWS), f32), pltpu.VMEM((8, ROWS), jnp.int32),
                  pltpu.VMEM((8, ROWS), f32), pltpu.SemaphoreType.DMA((4, 2)), pltpu.SemaphoreType.DMA((4, 2)))


def finish(lp, l, st_ref, out, s0, s1, s2, lpv, lv, ov, isem, jsem, osem, psem):
    n = lpv.shape[1]
    pieces = range(V // PIECE)

    def rows(k):
        return pl.ds(k * PIECE, PIECE)

    early = [pltpu.make_async_copy(lp.at[rows(k), pl.ds(0, n)], lpv.at[rows(k), :], isem.at[k]) for k in pieces]
    late = [pltpu.make_async_copy(l.at[rows(k), :], lv.at[rows(k), :], jsem.at[k]) for k in pieces]
    put = [pltpu.make_async_copy(lpv.at[rows(k), :], out.at[rows(k), pl.ds(0, n)], osem.at[k]) for k in pieces]
    end = [pltpu.make_async_copy(ov.at[rows(k), :], out.at[rows(k), pl.ds(n, ROWS)], psem.at[k]) for k in pieces]
    for k in pieces:
        early[k].start()
        late[k].start()
    s0[...] = st_ref[0:1, :]
    s1[...] = st_ref[1:2, :]
    s2[...] = st_ref[2:3, :]
    for k in pieces:
        early[k].wait()
        put[k].start()
        late[k].wait()
        r = k * PIECE
        ov[r:r + PIECE, :] = (lv[r:r + PIECE, :] - st_ref[0:1, n:]).astype(bf16)
        end[k].start()
    for k in pieces:
        put[k].wait()
        end[k].wait()


def solution(mesh):
    model_axes = ('tp2', 'tp')

    def local_step(hidden, w_gate, w_up, w_down, norm_gain, w_vocab, temperature, target_ids):
        n = hidden.shape[0]
        anyspec = pl.BlockSpec(memory_space=pl.ANY)
        vspec = pl.BlockSpec(memory_space=pltpu.VMEM)
        early, last_l, stats = pl.pallas_call(
            kernel,
            out_shape=(jax.ShapeDtypeStruct((V, n), bf16), jax.ShapeDtypeStruct((V, ROWS), f32),
                       jax.ShapeDtypeStruct((8, n), f32)),
            in_specs=[anyspec, anyspec, anyspec, anyspec, vspec, anyspec, vspec, vspec],
            out_specs=(anyspec, anyspec, vspec),
            scratch_shapes=[
                pltpu.VMEM((n, D), bf16),
                pltpu.VMEM((2, ROWS, D), bf16),
                pltpu.VMEM((2, ROWS // 2, D), bf16),
                pltpu.VMEM((2, 2, ROWS // 8, D), bf16),
                pltpu.VMEM((2, ROWS // 8, D), bf16),
                pltpu.VMEM((V, D), bf16),
                pltpu.VMEM((16, D), f32),
                pltpu.VMEM((CHUNKS, 8, ROWS), f32),
                pltpu.VMEM((CHUNKS, 8, 8, ROWS), f32),
                pltpu.SemaphoreType.DMA((CHUNKS, NK)),
                pltpu.SemaphoreType.DMA((CHUNKS, NK)),
                pltpu.SemaphoreType.DMA((CHUNKS, 8)),
                pltpu.SemaphoreType.DMA((CHUNKS, 8)),
                pltpu.SemaphoreType.DMA((CHUNKS,)),
                pltpu.SemaphoreType.DMA((4, 2)),
                pltpu.SemaphoreType.DMA((5,)),
                pltpu.SemaphoreType.REGULAR((3,)),
            ],
            compiler_params=pltpu.CompilerParams(collective_id=0, has_side_effects=True, vmem_limit_bytes=67043328),
        )(hidden, w_gate.T, w_up.T, w_down, norm_gain.reshape(1, D), w_vocab.T,
          temperature.reshape(1, n), target_ids.reshape(1, n))
        dma = pltpu.SemaphoreType.DMA((V // PIECE,))
        logprobs, s0, s1, s2 = pl.pallas_call(
            finish,
            out_shape=(jax.ShapeDtypeStruct((V, n), bf16),) + (jax.ShapeDtypeStruct((1, n), f32),) * 3,
            in_specs=[anyspec, anyspec, vspec],
            out_specs=(anyspec, vspec, vspec, vspec),
            scratch_shapes=[pltpu.VMEM((V, n - ROWS), bf16), pltpu.VMEM((V, ROWS), f32), pltpu.VMEM((V, ROWS), bf16),
                            dma, dma, dma, dma],
            compiler_params=pltpu.CompilerParams(vmem_limit_bytes=67043328),
        )(early, last_l, stats)
        return s0.reshape(n), s1.reshape(n), s2.reshape(n), logprobs.T

    return jax.shard_map(
        local_step, mesh=mesh,
        in_specs=(P('dp', None), P(None, model_axes), P(None, model_axes), P(model_axes, None),
                  P(None), P(None, model_axes), P('dp'), P('dp')),
        out_specs=(P('dp'), P('dp'), P('dp'), P('dp', model_axes)),
        check_vma=False)
```

```python
import functools

import jax
import jax.numpy as jnp
from jax import lax
from jax.experimental import pallas as pl
from jax.experimental.pallas import tpu as pltpu
from jax.sharding import PartitionSpec as P

NORM_EPS = 1e-6
ROWS = 256
CHUNKS = 4
D = 4096
PIECE = 400
WINDOW = 5
FF = 1376
V = 4000
GB = ((0, 256), (256, 256), (512, 512), (1024, 352))
VL = ((2752, 1248), (0, 1024), (1376, 1024), (1024, 352), (2400, 352))
VB = (((2752, 624), (3376, 624)), ((0, 512), (512, 512)), ((1376, 512), (1888, 512)), ((1024, 352), (2400, 352)))
VN = (1248, 1024, 1024, 704)
VR = (((2752, 0, 1248),), ((0, 0, 1024),), ((1376, 0, 1024),), ((1024, 0, 352), (2400, 352, 352)))
f32, bf16 = jnp.float32, jnp.bfloat16
MESH = pl.DeviceIdType.MESH

B1B_LATE = False
TABLE = {
    (1, 1, 0): [('E1a', 0)],
    (1, 1, 2): [('E1b', 0)],
    (1, 1, 3): [('E2a', 0)],
    (2, 1, 1): [('E2b', 0), ('E1a', 1)],
    (1, 2, 0): [('E3', 0)],
    (1, 2, 3): [('E1b', 1), ('E4', 0)],
    (2, 2, 0): [('E2a', 1), ('E5', 0)],
    (2, 2, 1): [('E2b', 1)],
    (1, 3, 0): [('E1a', 2), ('E3', 1)],
    (1, 3, 3): [('E1b', 2)],
    (2, 3, 1): [('E6', 0), ('E2a', 2), ('E4', 1)],
    (3, 0, 0): [('E2b', 2), ('E7', 0)],
    (3, 0, 1): [('E1a', 3), ('E5', 1)],
    (3, 0, 2): [('E1b', 3)],
    (3, 0, 3): [('E3', 2), ('E6', 1)],
    (3, 1, 0): [('E7', 1)],
    (3, 1, 1): [('E2a', 3), ('E2b', 3)],
    (3, 1, 2): [('E4', 2)],
    (3, 1, 3): [('E5', 2), ('E3', 3), ('E6', 2)],
    (3, 2, 0): [('E7', 2)],
    (3, 2, 1): [('E4', 3)],
    (3, 2, 3): [('E5', 3), ('E6', 3)],
    (3, 3, 0): [('E7', 3)],
}

KD, KB1A, KB1B, KB2, KA1, KA2A, KA2B, KA3A, KA3B, KA3C, KA3D = 0, 2, 4, 6, 8, 9, 10, 11, 12, 13, 14
NK = 15


def kernel(hid, wg, wu, wd, gain, wv, temp, tgt, out, last_l, stats,
           X, PB, DR, B1, B2, W, rsc, ST, SR,
           ssem, rsem, st_s, st_r, xsem, gsem, vsem, credit):
    dp = lax.axis_index('dp')
    y = lax.axis_index('tp2')
    tpi = lax.axis_index('tp')
    x = tpi // 2
    c = tpi % 2
    me = y * 4 + tpi
    f = x + c * (y - x)
    s = y + c * (x - y)
    partner = (dp, y, x * 2 + (1 - c))
    nbr1 = (dp, y + c * (1 - 2 * y), (x + (1 - c) * (1 - 2 * x)) * 2 + c)
    nbr2 = (dp, y + (1 - c) * (1 - 2 * y), (x + c * (1 - 2 * x)) * 2 + c)
    half = c * 128

    def al(v, n):
        return pl.multiple_of(v, n)

    def q(fp, sp):
        return al((2 * fp + sp) * 32, 32)

    def xload(i):
        return pltpu.make_async_copy(hid.at[pl.ds(i * ROWS, ROWS), :], X.at[pl.ds(i * ROWS, ROWS), :], xsem.at[i])

    def gload(b, k):
        src, base = ((wg, 0), (wu, FF))[k]
        r0, n = GB[b]
        return pltpu.make_async_copy(src.at[pl.ds(r0, n), :], W.at[pl.ds(base + r0, n), :], gsem.at[b, k])

    def vload(t):
        r0, n = VL[t]
        return pltpu.make_async_copy(wv.at[pl.ds(r0, n), :], W.at[pl.ds(r0, n), :], vsem.at[t])

    def remote(src, dst, i, k, dev):
        return pltpu.make_async_remote_copy(src_ref=src, dst_ref=dst, send_sem=ssem.at[i, k], recv_sem=rsem.at[i, k],
                                            device_id=dev, device_id_type=MESH)

    def xrows(i, fp, sp, hb):
        return X.at[pl.ds(al(i * ROWS + hb + q(fp, sp), 32), 32), :]

    def prow(i, fp, sp, cs):
        return PB.at[lax.rem(i, 2), pl.ds(al(half + q(fp, sp), 32), 32), cs]

    def copy(i, k):
        sl = lax.rem(i, 2)
        if k < KA1:
            kind = k - k % 2
            cs = pl.ds(2048 * (k % 2), 2048)
            if kind == KD:
                return remote(PB.at[sl, pl.ds(al(128 - half, 128), 128), cs], DR.at[sl, :, cs], i, k, partner)
            if kind == KB1A:
                return remote(prow(i, 1 - f, 1 - s, cs), B1.at[sl, 0, :, cs], i, k, nbr1)
            if kind == KB1B:
                return remote(prow(i, 1 - f, s, cs), B1.at[sl, 1, :, cs], i, k, nbr1)
            return remote(prow(i, f, 1 - s, cs), B2.at[sl, :, cs], i, k, nbr2)
        fp, sp = {KA1: (f, s), KA2A: (f, s), KA3A: (f, s), KA2B: (f, 1 - s), KA3B: (f, 1 - s),
                  KA3C: (1 - f, s), KA3D: (1 - f, 1 - s)}[k]
        dev = {KA1: nbr2, KA2A: nbr1, KA2B: nbr1}.get(k, partner)
        r = xrows(i, fp, sp, half)
        return remote(r, r, i, k, dev)

    def e1(i, h):
        copy(i, KD + h).wait_recv()
        sl = lax.rem(i, 2)
        for sp, k in ((1 - s, KB1A), (s, KB1B)):
            r0 = q(1 - f, sp)

            def add(t, carry):
                pr = pl.ds(al(half + r0 + t * 16, 16), 16)
                dr = pl.ds(al(r0 + t * 16, 16), 16)
                for cb in range(2):
                    cs = slice(2048 * h + cb * 1024, 2048 * h + cb * 1024 + 1024)
                    PB[sl, pr, cs] = (PB[sl, pr, cs].astype(f32) + DR[sl, dr, cs].astype(f32)).astype(bf16)
                return carry

            lax.fori_loop(0, 2, add, 0)
            if k == KB1A and i >= 2 and h == 0:
                pl.semaphore_wait(credit.at[1], 1)
            if k == KB1A or not B1B_LATE:
                copy(i, k + h).start()

    def e2(i, h):
        copy(i, KB1A + h).wait_recv()
        sl = lax.rem(i, 2)
        r0 = q(f, 1 - s)

        def add(t, carry):
            pr = pl.ds(al(half + r0 + t * 16, 16), 16)
            dr = pl.ds(al(r0 + t * 16, 16), 16)
            br = pl.ds(al(t * 16, 16), 16)
            for cb in range(2):
                cs = slice(2048 * h + cb * 1024, 2048 * h + cb * 1024 + 1024)
                PB[sl, pr, cs] = (PB[sl, pr, cs].astype(f32) + DR[sl, dr, cs].astype(f32)
                                  + B1[sl, 0, br, cs].astype(f32)).astype(bf16)
            return carry

        lax.fori_loop(0, 2, add, 0)
        if i >= 2 and h == 0:
            pl.semaphore_wait(credit.at[2], 1)
        copy(i, KB2 + h).start()
        if B1B_LATE:
            copy(i, KB1B + h).start()

    def e3(i):
        for h in range(2):
            copy(i, KB1B + h).wait_recv()
            copy(i, KB2 + h).wait_recv()
        sl = lax.rem(i, 2)
        r0 = q(f, s)

        def fin(t, carry):
            pr = pl.ds(al(half + r0 + t * 16, 16), 16)
            dr = pl.ds(al(r0 + t * 16, 16), 16)
            br = pl.ds(al(t * 16, 16), 16)
            xr = pl.ds(al(i * ROWS + half + r0 + t * 16, 16), 16)
            acc = jnp.zeros((16, 128), f32)
            for cb in range(16):
                cs = slice(cb * 256, cb * 256 + 256)
                part = (PB[sl, pr, cs].astype(f32) + DR[sl, dr, cs].astype(f32)
                        + B1[sl, 1, br, cs].astype(f32) + B2[sl, br, cs].astype(f32)).astype(bf16)
                r = X[xr, cs].astype(f32) + part.astype(f32)
                rsc[:, cs] = r
                sq = r * r
                acc = acc + sq[:, :128] + sq[:, 128:]
            ms = jnp.sum(acc, axis=1, keepdims=True) * (1.0 / D)
            inv = lax.rsqrt(ms + NORM_EPS)
            for cb in range(16):
                cs = slice(cb * 256, cb * 256 + 256)
                X[xr, cs] = (gain[:, cs] * rsc[:, cs] * inv).astype(bf16)
            return carry

        lax.fori_loop(0, 2, fin, 0)
        copy(i, KA1).start()
        copy(i, KA2A).start()
        copy(i, KA3A).start()
        if i < 2:
            for n, dev in ((0, partner), (1, nbr1), (2, nbr2)):
                pl.semaphore_signal(credit.at[n], inc=1, device_id=dev, device_id_type=MESH)

    def e4(i):
        copy(i, KA1).wait_recv()
        copy(i, KA2B).start()
        copy(i, KA3B).start()

    def e5(i):
        copy(i, KA2A).wait_recv()
        copy(i, KA3C).start()

    def e6(i):
        copy(i, KA2B).wait_recv()
        copy(i, KA3D).start()

    def e7(i):
        for k in (KA3A, KA3B, KA3C, KA3D):
            copy(i, k).wait_recv()

    events = {'E3': e3, 'E4': e4, 'E5': e5, 'E6': e6, 'E7': e7}
    for h_, n_ in ((0, 'a'), (1, 'b')):
        events['E1' + n_] = functools.partial(e1, h=h_)
        events['E2' + n_] = functools.partial(e2, h=h_)

    def progress(phase, i, b):
        for ck in range(CHUNKS):
            todo = TABLE.get((phase, ck, b), [])
            if todo:
                @pl.when(i == ck)
                def _():
                    for name, cc in todo:
                        with jax.named_scope(f'{name}_{cc}'):
                            events[name](cc)

    xload(0).start()
    for b in range(2):
        for k in range(2):
            gload(b, k).start()

    def dott(w, xv):
        return lax.dot_general(w, xv, (((1,), (1,)), ((), ())), preferred_element_type=f32)

    def phase1(wdv, act, dsem):
        def dload(k):
            cs = pl.ds(2048 * k, 2048)
            return pltpu.make_async_copy(wd.at[:, cs], wdv.at[:, cs], dsem.at[k])


        bar = pltpu.get_barrier_semaphore()
        for d in range(1, 8):
            o = (me + d) % 8
            pl.semaphore_signal(bar, inc=1, device_id=(dp, o // 4, o % 4), device_id_type=MESH)
        pl.semaphore_wait(bar, 7)
        for k in range(2):
            gload(2, k).start()

        def chunk(i, carry):
            rows = pl.ds(al(i * ROWS, ROWS), ROWS)
            sl = lax.rem(i, 2)
            xload(i).wait()

            def first(fn):
                pl.when(i == 0)(fn)

            def last(fn):
                pl.when(i == CHUNKS - 1)(fn)

            for b, (r0, n) in enumerate(GB):
                @first
                def _():
                    for k in range(2):
                        gload(b, k).wait()
                    for cp in ((gload(3, 0), gload(3, 1)), (dload(0), dload(1)), (xload(1), xload(2), xload(3)), ())[b]:
                        cp.start()

                progress(1, i, b)
                with jax.named_scope(f'G{b}'):
                    g = dott(W[r0:r0 + n, :], X[rows, :])
                    u = dott(W[FF + r0:FF + r0 + n, :], X[rows, :])
                    h = g * jax.nn.sigmoid(g) * u
                    act[:, r0:r0 + n] = jnp.transpose(h.astype(bf16))

                @last
                def _():
                    for t in ((), (), (1, 2), (3, 4))[b]:
                        vload(t).start()

            @first
            def _():
                vload(0).start()

            for b in range(2):
                first(lambda: dload(b).wait())
                progress(2, i, b)
                if b == 0:
                    @pl.when(i >= 2)
                    def _():
                        for k in range(KA1):
                            copy(i - 2, k).wait_send()
                        pl.semaphore_wait(credit.at[0], 1)

                with jax.named_scope(f'D{b}'):
                    for n in range(8):
                        cs = slice(2048 * b + 256 * n, 2048 * b + 256 * n + 256)
                        PB[sl, :, cs] = jnp.dot(act[...], wdv[:, cs], preferred_element_type=f32).astype(bf16)

                copy(i, KD + b).start()

            return carry

        lax.fori_loop(0, CHUNKS, chunk, 0)

    pl.run_scoped(phase1, pltpu.VMEM((FF, D), bf16), pltpu.VMEM((ROWS, FF), bf16), pltpu.SemaphoreType.DMA((2,)))

    def phase2(L0, L1, L2, L3, OS, state, IT, TG, LN, osem, lsem):
        L = (L0, L1, L2, L3)
        sub = lax.broadcasted_iota(jnp.int32, (8, ROWS), 0)

        def stats_block(cur, b):
            groups = [(lo + k, v + k) for v, lo, n in VR[b] for k in range(0, n, 8)]
            ms = [L[b][cur, r:r + 8, :] for r, _ in groups[:4]]
            for k, (r, _) in enumerate(groups[4:]):
                ms[k % 4] = jnp.maximum(ms[k % 4], L[b][cur, r:r + 8, :])
            m_new = jnp.maximum(jnp.maximum(ms[0], ms[1]), jnp.maximum(ms[2], ms[3]))
            zero = jnp.zeros((8, ROWS), f32)
            ss, ws, ts = [zero] * 2, [zero] * 2, [zero] * 2
            if b > 0:
                m_old = state[0]
                m_new = jnp.maximum(m_new, m_old)
                scale = jnp.exp(m_old - m_new)
                ss[0], ws[0], ts[0] = state[1] * scale, state[2] * scale, state[3]
            tg = TG[...] - sub
            for k, (r, v) in enumerate(groups):
                l = L[b][cur, r:r + 8, :]
                e = jnp.exp(l - m_new)
                ss[k % 2] = ss[k % 2] + e
                ws[k % 2] = ws[k % 2] + e * l
                ts[k % 2] = jnp.where(tg == v, l, ts[k % 2])
            state[0] = m_new
            state[1] = ss[0] + ss[1]
            state[2] = ws[0] + ws[1]
            state[3] = ts[0] + ts[1]

        def final_block(old, b):
            for v, lo, n in VR[b]:
                for k in range(0, n, 16):
                    OS[v + k:v + k + 16, :] = (L[b][old, lo + k:lo + k + 16, :] - LN[0:1, :]).astype(bf16)

        def ocopies(i, blocks):
            return [pltpu.make_async_copy(OS.at[pl.ds(v, n), :], out.at[pl.ds(v, n), pl.ds(al(i * ROWS, ROWS), ROWS)],
                                          osem.at[b, k]) for b in blocks for k, (v, lo, n) in enumerate(VR[b])]

        def lcopies(b):
            return [pltpu.make_async_copy(L[b].at[(CHUNKS - 1) % 2, pl.ds(lo, n), :], last_l.at[pl.ds(v, n), :], lsem.at[b, k])
                    for k, (v, lo, n) in enumerate(VR[b])]

        def stat_copy(i, d):
            o = (me + d) % 8
            return pltpu.make_async_remote_copy(src_ref=ST.at[i], dst_ref=SR.at[i, me], send_sem=st_s.at[i, d],
                                                recv_sem=st_r.at[i, me],
                                                device_id=(dp, o // 4, o % 4), device_id_type=MESH)

        def stat_wait(i, d):
            o = (me + d) % 8
            return pltpu.make_async_remote_copy(src_ref=ST.at[i], dst_ref=SR.at[i, o], send_sem=st_s.at[i, d],
                                                recv_sem=st_r.at[i, o],
                                                device_id=(dp, o // 4, o % 4), device_id_type=MESH)

        def send_stats(i):
            m = state[0]
            mx = jnp.max(m, axis=0, keepdims=True)
            e = jnp.exp(m - mx)
            row = lax.broadcasted_iota(jnp.int32, (8, ROWS), 0)
            pk = jnp.broadcast_to(mx, (8, ROWS))
            for n in (1, 2, 3):
                v = state[n] * e if n < 3 else state[n]
                pk = jnp.where(row == n, jnp.sum(v, axis=0, keepdims=True), pk)
            ST[i] = pk
            SR[i, me] = pk
            for d in range(1, 8):
                stat_copy(i, d).start()

        def recv_stats(i):
            for d in range(1, 8):
                stat_wait(i, d).wait_recv()
            parts = [SR[i, o] for o in range(8)]
            mg = parts[0][0:1, :]
            for p_ in parts[1:]:
                mg = jnp.maximum(mg, p_[0:1, :])
            sg = wgt = tl = jnp.zeros((1, ROWS), f32)
            for p_ in parts:
                e = jnp.exp(p_[0:1, :] - mg)
                sg = sg + p_[1:2, :] * e
                wgt = wgt + p_[2:3, :] * e
                tl = tl + p_[3:4, :]
            lg = mg + jnp.log(sg)
            cs = pl.ds(al(i * ROWS, ROWS), ROWS)
            stats[0:1, cs] = lg
            stats[1:2, cs] = lg - wgt / sg
            stats[2:3, cs] = tl - lg
            LN[...] = jnp.broadcast_to(lg, (8, ROWS))

        def chunk(j, carry):
            rows = pl.ds(al(j * ROWS, ROWS), ROWS)
            cur, old = lax.rem(j, 2), lax.rem(j + 1, 2)
            cs = pl.ds(al(j * ROWS, ROWS), ROWS)
            IT[...] = jnp.broadcast_to(1.0 / temp[:, cs], (8, ROWS))
            tid = tgt[:, cs] - me * V
            TG[...] = jnp.broadcast_to(tid, (8, ROWS))

            def vblock(b):
                lo = 0
                for r0, n in VB[b]:
                    L[b][cur, lo:lo + n, :] = dott(W[r0:r0 + n, :], X[rows, :]) * IT[0:1, :]
                    lo += n

            for b in range(4):
                @pl.when(j == 0)
                def _():
                    for t in ((0,), (1,), (2,), (3, 4))[b]:
                        vload(t).wait()

                progress(3, j, b)
                if b == 3:
                    @pl.when(j >= 2)
                    def _():
                        for cp in ocopies(j - 2, range(4)):
                            cp.wait()

                    @pl.when(j >= 1)
                    def _():
                        with jax.named_scope('RST'):
                            recv_stats(j - 1)

                with jax.named_scope(f'V{b}'):
                    vblock(b)
                    if b >= 1:
                        stats_block(cur, b - 1)
                if b == 3:
                    done = range(4)
                    for d in done:
                        final_block(old, d)

                    @pl.when(j >= 1)
                    def _():
                        for cp in ocopies(j - 1, done):
                            cp.start()

                @pl.when(j == CHUNKS - 1)
                def _():
                    for cp in lcopies(b):
                        cp.start()

            with jax.named_scope('STL'):
                stats_block(cur, 3)
                send_stats(j)
            return carry

        lax.fori_loop(0, CHUNKS, chunk, 0)
        for i in range(CHUNKS):
            for k in range(NK):
                if k >= KA1 or i >= 2:
                    copy(i, k).wait_send()
        for cp in ocopies(CHUNKS - 2, range(4)):
            cp.wait()
        for b in range(4):
            for cp in lcopies(b):
                cp.wait()
        with jax.named_scope('RSTL'):
            recv_stats(CHUNKS - 1)
        for i in range(CHUNKS):
            for d in range(1, 8):
                stat_copy(i, d).wait_send()

    pl.run_scoped(phase2, *[pltpu.VMEM((2, n, ROWS), f32) for n in VN], pltpu.VMEM((V, ROWS), bf16),
                  pltpu.VMEM((4, 8, ROWS), f32), pltpu.VMEM((8, ROWS), f32), pltpu.VMEM((8, ROWS), jnp.int32),
                  pltpu.VMEM((8, ROWS), f32), pltpu.SemaphoreType.DMA((4, 2)), pltpu.SemaphoreType.DMA((4, 2)))


def finish(lp, l, st_ref, out, s0, s1, s2, lpv, lv, ov, isem, jsem, osem, psem):
    n = lpv.shape[1]
    pieces = range(V // PIECE)

    def rows(k):
        return pl.ds(k * PIECE, PIECE)

    early = [pltpu.make_async_copy(lp.at[rows(k), pl.ds(0, n)], lpv.at[rows(k), :], isem.at[k]) for k in pieces]
    late = [pltpu.make_async_copy(l.at[rows(k), :], lv.at[rows(k), :], jsem.at[k]) for k in pieces]
    put = [pltpu.make_async_copy(lpv.at[rows(k), :], out.at[rows(k), pl.ds(0, n)], osem.at[k]) for k in pieces]
    end = [pltpu.make_async_copy(ov.at[rows(k), :], out.at[rows(k), pl.ds(n, ROWS)], psem.at[k]) for k in pieces]
    for k in pieces[:WINDOW]:
        early[k].start()
        late[k].start()
    s0[...] = st_ref[0:1, :]
    s1[...] = st_ref[1:2, :]
    s2[...] = st_ref[2:3, :]
    for k in pieces:
        early[k].wait()
        put[k].start()
        late[k].wait()
        if k + WINDOW < len(pieces):
            early[k + WINDOW].start()
            late[k + WINDOW].start()
        r = k * PIECE
        ov[r:r + PIECE, :] = (lv[r:r + PIECE, :] - st_ref[0:1, n:]).astype(bf16)
        end[k].start()
    for k in pieces:
        put[k].wait()
        end[k].wait()


def solution(mesh):
    model_axes = ('tp2', 'tp')

    def local_step(hidden, w_gate, w_up, w_down, norm_gain, w_vocab, temperature, target_ids):
        n = hidden.shape[0]
        anyspec = pl.BlockSpec(memory_space=pl.ANY)
        vspec = pl.BlockSpec(memory_space=pltpu.VMEM)
        early, last_l, stats = pl.pallas_call(
            kernel,
            out_shape=(jax.ShapeDtypeStruct((V, n), bf16), jax.ShapeDtypeStruct((V, ROWS), f32),
                       jax.ShapeDtypeStruct((8, n), f32)),
            in_specs=[anyspec, anyspec, anyspec, anyspec, vspec, anyspec, vspec, vspec],
            out_specs=(anyspec, anyspec, vspec),
            scratch_shapes=[
                pltpu.VMEM((n, D), bf16),
                pltpu.VMEM((2, ROWS, D), bf16),
                pltpu.VMEM((2, ROWS // 2, D), bf16),
                pltpu.VMEM((2, 2, ROWS // 8, D), bf16),
                pltpu.VMEM((2, ROWS // 8, D), bf16),
                pltpu.VMEM((V, D), bf16),
                pltpu.VMEM((16, D), f32),
                pltpu.VMEM((CHUNKS, 8, ROWS), f32),
                pltpu.VMEM((CHUNKS, 8, 8, ROWS), f32),
                pltpu.SemaphoreType.DMA((CHUNKS, NK)),
                pltpu.SemaphoreType.DMA((CHUNKS, NK)),
                pltpu.SemaphoreType.DMA((CHUNKS, 8)),
                pltpu.SemaphoreType.DMA((CHUNKS, 8)),
                pltpu.SemaphoreType.DMA((CHUNKS,)),
                pltpu.SemaphoreType.DMA((4, 2)),
                pltpu.SemaphoreType.DMA((5,)),
                pltpu.SemaphoreType.REGULAR((3,)),
            ],
            compiler_params=pltpu.CompilerParams(collective_id=0, has_side_effects=True, vmem_limit_bytes=67043328),
        )(hidden, w_gate.T, w_up.T, w_down, norm_gain.reshape(1, D), w_vocab.T,
          temperature.reshape(1, n), target_ids.reshape(1, n))
        dma = pltpu.SemaphoreType.DMA((V // PIECE,))
        logprobs, s0, s1, s2 = pl.pallas_call(
            finish,
            out_shape=(jax.ShapeDtypeStruct((V, n), bf16),) + (jax.ShapeDtypeStruct((1, n), f32),) * 3,
            in_specs=[anyspec, anyspec, vspec],
            out_specs=(anyspec, vspec, vspec, vspec),
            scratch_shapes=[pltpu.VMEM((V, n - ROWS), bf16), pltpu.VMEM((V, ROWS), f32), pltpu.VMEM((V, ROWS), bf16),
                            dma, dma, dma, dma],
            compiler_params=pltpu.CompilerParams(vmem_limit_bytes=67043328),
        )(early, last_l, stats)
        return s0.reshape(n), s1.reshape(n), s2.reshape(n), logprobs.T

    return jax.shard_map(
        local_step, mesh=mesh,
        in_specs=(P('dp', None), P(None, model_axes), P(None, model_axes), P(model_axes, None),
                  P(None), P(None, model_axes), P('dp'), P('dp')),
        out_specs=(P('dp'), P('dp'), P('dp'), P('dp', model_axes)),
        check_vma=False)
```

```python
import functools

import jax
import jax.numpy as jnp
from jax import lax
from jax.experimental import pallas as pl
from jax.experimental.pallas import tpu as pltpu
from jax.sharding import PartitionSpec as P

NORM_EPS = 1e-6
ROWS = 256
CHUNKS = 4
D = 4096
PIECE = 400
FF = 1376
V = 4000
GB = ((0, 256), (256, 256), (512, 512), (1024, 352))
VL = ((2752, 1248), (0, 1024), (1376, 1024), (1024, 352), (2400, 352))
VB = (((2752, 624), (3376, 624)), ((0, 512), (512, 512)), ((1376, 512), (1888, 512)), ((1024, 352), (2400, 352)))
VN = (1248, 1024, 1024, 704)
VR = (((2752, 0, 1248),), ((0, 0, 1024),), ((1376, 0, 1024),), ((1024, 0, 352), (2400, 352, 352)))
f32, bf16 = jnp.float32, jnp.bfloat16
MESH = pl.DeviceIdType.MESH

B1B_LATE = False
TABLE = {
    (1, 1, 0): [('E1a', 0)],
    (1, 1, 2): [('E1b', 0)],
    (1, 1, 3): [('E2a', 0)],
    (1, 2, 0): [('E3', 0)],
    (1, 2, 2): [('E1b', 1)],
    (1, 3, 1): [('E3', 1)],
    (2, 1, 1): [('E2b', 0), ('E1a', 1)],
    (2, 2, 0): [('E2a', 1), ('E4', 0)],
    (2, 2, 1): [('E2b', 1), ('E1a', 2)],
    (2, 3, 0): [('E1b', 2), ('E5', 0)],
    (2, 3, 1): [('E2a', 2), ('E6', 0)],
    (3, 0, 0): [('E7', 0), ('E4', 1)],
    (3, 0, 1): [('E2b', 2), ('E1a', 3)],
    (3, 0, 2): [('E1b', 3), ('E5', 1)],
    (3, 0, 3): [('E6', 1), ('E3', 2)],
    (3, 1, 0): [('E7', 1)],
    (3, 1, 1): [('E2a', 3), ('E2b', 3)],
    (3, 1, 2): [('E4', 2)],
    (3, 1, 3): [('E5', 2), ('E3', 3)],
    (3, 2, 0): [('E6', 2), ('E7', 2)],
    (3, 2, 1): [('E4', 3)],
    (3, 2, 2): [('E5', 3)],
    (3, 2, 3): [('E6', 3)],
    (3, 3, 0): [('E7', 3)],
}

KD, KB1A, KB1B, KB2, KA1, KA2A, KA2B, KA3A, KA3B, KA3C, KA3D = 0, 2, 4, 6, 8, 9, 10, 11, 12, 13, 14
NK = 15


def kernel(hid, wg, wu, wd, gain, wv, temp, tgt, out, last_l, stats,
           X, PB, DR, B1, B2, W, rsc, ST, SR,
           ssem, rsem, st_s, st_r, xsem, gsem, vsem, credit):
    dp = lax.axis_index('dp')
    y = lax.axis_index('tp2')
    tpi = lax.axis_index('tp')
    x = tpi // 2
    c = tpi % 2
    me = y * 4 + tpi
    f = x + c * (y - x)
    s = y + c * (x - y)
    partner = (dp, y, x * 2 + (1 - c))
    nbr1 = (dp, y + c * (1 - 2 * y), (x + (1 - c) * (1 - 2 * x)) * 2 + c)
    nbr2 = (dp, y + (1 - c) * (1 - 2 * y), (x + c * (1 - 2 * x)) * 2 + c)
    half = c * 128

    def al(v, n):
        return pl.multiple_of(v, n)

    def q(fp, sp):
        return al((2 * fp + sp) * 32, 32)

    def xload(i):
        return pltpu.make_async_copy(hid.at[pl.ds(i * ROWS, ROWS), :], X.at[pl.ds(i * ROWS, ROWS), :], xsem.at[i])

    def gload(b, k):
        src, base = ((wg, 0), (wu, FF))[k]
        r0, n = GB[b]
        return pltpu.make_async_copy(src.at[pl.ds(r0, n), :], W.at[pl.ds(base + r0, n), :], gsem.at[b, k])

    def vload(t):
        r0, n = VL[t]
        return pltpu.make_async_copy(wv.at[pl.ds(r0, n), :], W.at[pl.ds(r0, n), :], vsem.at[t])

    def remote(src, dst, i, k, dev):
        return pltpu.make_async_remote_copy(src_ref=src, dst_ref=dst, send_sem=ssem.at[i, k], recv_sem=rsem.at[i, k],
                                            device_id=dev, device_id_type=MESH)

    def xrows(i, fp, sp, hb):
        return X.at[pl.ds(al(i * ROWS + hb + q(fp, sp), 32), 32), :]

    def prow(i, fp, sp, cs):
        return PB.at[lax.rem(i, 2), pl.ds(al(half + q(fp, sp), 32), 32), cs]

    def copy(i, k):
        sl = lax.rem(i, 2)
        if k < KA1:
            kind = k - k % 2
            cs = pl.ds(2048 * (k % 2), 2048)
            if kind == KD:
                return remote(PB.at[sl, pl.ds(al(128 - half, 128), 128), cs], DR.at[sl, :, cs], i, k, partner)
            if kind == KB1A:
                return remote(prow(i, 1 - f, 1 - s, cs), B1.at[sl, 0, :, cs], i, k, nbr1)
            if kind == KB1B:
                return remote(prow(i, 1 - f, s, cs), B1.at[sl, 1, :, cs], i, k, nbr1)
            return remote(prow(i, f, 1 - s, cs), B2.at[sl, :, cs], i, k, nbr2)
        fp, sp = {KA1: (f, s), KA2A: (f, s), KA3A: (f, s), KA2B: (f, 1 - s), KA3B: (f, 1 - s),
                  KA3C: (1 - f, s), KA3D: (1 - f, 1 - s)}[k]
        dev = {KA1: nbr2, KA2A: nbr1, KA2B: nbr1}.get(k, partner)
        r = xrows(i, fp, sp, half)
        return remote(r, r, i, k, dev)

    def e1(i, h):
        copy(i, KD + h).wait_recv()
        sl = lax.rem(i, 2)
        for sp, k in ((1 - s, KB1A), (s, KB1B)):
            r0 = q(1 - f, sp)

            def add(t, carry):
                pr = pl.ds(al(half + r0 + t * 16, 16), 16)
                dr = pl.ds(al(r0 + t * 16, 16), 16)
                for cb in range(2):
                    cs = slice(2048 * h + cb * 1024, 2048 * h + cb * 1024 + 1024)
                    PB[sl, pr, cs] = (PB[sl, pr, cs].astype(f32) + DR[sl, dr, cs].astype(f32)).astype(bf16)
                return carry

            lax.fori_loop(0, 2, add, 0)
            if k == KB1A and i >= 2 and h == 0:
                pl.semaphore_wait(credit.at[1], 1)
            if k == KB1A or not B1B_LATE:
                copy(i, k + h).start()

    def e2(i, h):
        copy(i, KB1A + h).wait_recv()
        sl = lax.rem(i, 2)
        r0 = q(f, 1 - s)

        def add(t, carry):
            pr = pl.ds(al(half + r0 + t * 16, 16), 16)
            dr = pl.ds(al(r0 + t * 16, 16), 16)
            br = pl.ds(al(t * 16, 16), 16)
            for cb in range(2):
                cs = slice(2048 * h + cb * 1024, 2048 * h + cb * 1024 + 1024)
                PB[sl, pr, cs] = (PB[sl, pr, cs].astype(f32) + DR[sl, dr, cs].astype(f32)
                                  + B1[sl, 0, br, cs].astype(f32)).astype(bf16)
            return carry

        lax.fori_loop(0, 2, add, 0)
        if i >= 2 and h == 0:
            pl.semaphore_wait(credit.at[2], 1)
        copy(i, KB2 + h).start()
        if B1B_LATE:
            copy(i, KB1B + h).start()

    def e3(i):
        for h in range(2):
            copy(i, KB1B + h).wait_recv()
            copy(i, KB2 + h).wait_recv()
        sl = lax.rem(i, 2)
        r0 = q(f, s)

        def fin(t, carry):
            pr = pl.ds(al(half + r0 + t * 16, 16), 16)
            dr = pl.ds(al(r0 + t * 16, 16), 16)
            br = pl.ds(al(t * 16, 16), 16)
            xr = pl.ds(al(i * ROWS + half + r0 + t * 16, 16), 16)
            acc = jnp.zeros((16, 128), f32)
            for cb in range(16):
                cs = slice(cb * 256, cb * 256 + 256)
                part = (PB[sl, pr, cs].astype(f32) + DR[sl, dr, cs].astype(f32)
                        + B1[sl, 1, br, cs].astype(f32) + B2[sl, br, cs].astype(f32)).astype(bf16)
                r = X[xr, cs].astype(f32) + part.astype(f32)
                rsc[:, cs] = r
                sq = r * r
                acc = acc + sq[:, :128] + sq[:, 128:]
            ms = jnp.sum(acc, axis=1, keepdims=True) * (1.0 / D)
            inv = lax.rsqrt(ms + NORM_EPS)
            for cb in range(16):
                cs = slice(cb * 256, cb * 256 + 256)
                X[xr, cs] = (gain[:, cs] * rsc[:, cs] * inv).astype(bf16)
            return carry

        lax.fori_loop(0, 2, fin, 0)
        copy(i, KA1).start()
        copy(i, KA2A).start()
        copy(i, KA3A).start()
        if i < 2:
            for n, dev in ((0, partner), (1, nbr1), (2, nbr2)):
                pl.semaphore_signal(credit.at[n], inc=1, device_id=dev, device_id_type=MESH)

    def e4(i):
        copy(i, KA1).wait_recv()
        copy(i, KA2B).start()
        copy(i, KA3B).start()

    def e5(i):
        copy(i, KA2A).wait_recv()
        copy(i, KA3C).start()

    def e6(i):
        copy(i, KA2B).wait_recv()
        copy(i, KA3D).start()

    def e7(i):
        for k in (KA3A, KA3B, KA3C, KA3D):
            copy(i, k).wait_recv()

    events = {'E3': e3, 'E4': e4, 'E5': e5, 'E6': e6, 'E7': e7}
    for h_, n_ in ((0, 'a'), (1, 'b')):
        events['E1' + n_] = functools.partial(e1, h=h_)
        events['E2' + n_] = functools.partial(e2, h=h_)

    def progress(phase, i, b):
        for ck in range(CHUNKS):
            todo = TABLE.get((phase, ck, b), [])
            if todo:
                @pl.when(i == ck)
                def _():
                    for name, cc in todo:
                        events[name](cc)

    xload(0).start()
    for b in range(2):
        for k in range(2):
            gload(b, k).start()

    def dott(w, xv):
        return lax.dot_general(w, xv, (((1,), (1,)), ((), ())), preferred_element_type=f32)

    def phase1(wdv, act, dsem):
        def dload(k):
            cs = pl.ds(2048 * k, 2048)
            return pltpu.make_async_copy(wd.at[:, cs], wdv.at[:, cs], dsem.at[k])


        bar = pltpu.get_barrier_semaphore()
        for d in range(1, 8):
            o = (me + d) % 8
            pl.semaphore_signal(bar, inc=1, device_id=(dp, o // 4, o % 4), device_id_type=MESH)
        pl.semaphore_wait(bar, 7)
        for k in range(2):
            gload(2, k).start()

        def chunk(i, carry):
            rows = pl.ds(al(i * ROWS, ROWS), ROWS)
            sl = lax.rem(i, 2)
            xload(i).wait()

            def first(fn):
                pl.when(i == 0)(fn)

            def last(fn):
                pl.when(i == CHUNKS - 1)(fn)

            for b, (r0, n) in enumerate(GB):
                @first
                def _():
                    for k in range(2):
                        gload(b, k).wait()
                    for cp in ((gload(3, 0), gload(3, 1)), (dload(0), dload(1)), (xload(1), xload(2), xload(3)), ())[b]:
                        cp.start()

                progress(1, i, b)
                g = dott(W[r0:r0 + n, :], X[rows, :])
                u = dott(W[FF + r0:FF + r0 + n, :], X[rows, :])
                h = g * jax.nn.sigmoid(g) * u
                act[:, r0:r0 + n] = jnp.transpose(h.astype(bf16))

                @last
                def _():
                    for t in ((), (), (1, 2), (3, 4))[b]:
                        vload(t).start()

            @first
            def _():
                vload(0).start()

            for b in range(2):
                first(lambda: dload(b).wait())
                progress(2, i, b)
                if b == 0:
                    @pl.when(i >= 2)
                    def _():
                        for k in range(KA1):
                            copy(i - 2, k).wait_send()
                        pl.semaphore_wait(credit.at[0], 1)

                for n in range(8):
                    cs = slice(2048 * b + 256 * n, 2048 * b + 256 * n + 256)
                    PB[sl, :, cs] = jnp.dot(act[...], wdv[:, cs], preferred_element_type=f32).astype(bf16)

                copy(i, KD + b).start()

            return carry

        lax.fori_loop(0, CHUNKS, chunk, 0)

    pl.run_scoped(phase1, pltpu.VMEM((FF, D), bf16), pltpu.VMEM((ROWS, FF), bf16), pltpu.SemaphoreType.DMA((2,)))

    def phase2(L0, L1, L2, L3, OS, state, IT, TG, LN, osem, lsem):
        L = (L0, L1, L2, L3)
        sub = lax.broadcasted_iota(jnp.int32, (8, ROWS), 0)

        def stats_block(cur, b):
            groups = [(lo + k, v + k) for v, lo, n in VR[b] for k in range(0, n, 8)]
            ms = [L[b][cur, r:r + 8, :] for r, _ in groups[:4]]
            for k, (r, _) in enumerate(groups[4:]):
                ms[k % 4] = jnp.maximum(ms[k % 4], L[b][cur, r:r + 8, :])
            m_new = jnp.maximum(jnp.maximum(ms[0], ms[1]), jnp.maximum(ms[2], ms[3]))
            zero = jnp.zeros((8, ROWS), f32)
            ss, ws, ts = [zero] * 2, [zero] * 2, [zero] * 2
            if b > 0:
                m_old = state[0]
                m_new = jnp.maximum(m_new, m_old)
                scale = jnp.exp(m_old - m_new)
                ss[0], ws[0], ts[0] = state[1] * scale, state[2] * scale, state[3]
            tg = TG[...] - sub
            for k, (r, v) in enumerate(groups):
                l = L[b][cur, r:r + 8, :]
                e = jnp.exp(l - m_new)
                ss[k % 2] = ss[k % 2] + e
                ws[k % 2] = ws[k % 2] + e * l
                ts[k % 2] = jnp.where(tg == v, l, ts[k % 2])
            state[0] = m_new
            state[1] = ss[0] + ss[1]
            state[2] = ws[0] + ws[1]
            state[3] = ts[0] + ts[1]

        def final_block(old, b):
            for v, lo, n in VR[b]:
                for k in range(0, n, 16):
                    OS[v + k:v + k + 16, :] = (L[b][old, lo + k:lo + k + 16, :] - LN[0:1, :]).astype(bf16)

        def ocopies(i, blocks):
            return [pltpu.make_async_copy(OS.at[pl.ds(v, n), :], out.at[pl.ds(v, n), pl.ds(al(i * ROWS, ROWS), ROWS)],
                                          osem.at[b, k]) for b in blocks for k, (v, lo, n) in enumerate(VR[b])]

        def lcopies(b):
            return [pltpu.make_async_copy(L[b].at[(CHUNKS - 1) % 2, pl.ds(lo, n), :], last_l.at[pl.ds(v, n), :], lsem.at[b, k])
                    for k, (v, lo, n) in enumerate(VR[b])]

        def stat_copy(i, d):
            o = (me + d) % 8
            return pltpu.make_async_remote_copy(src_ref=ST.at[i], dst_ref=SR.at[i, me], send_sem=st_s.at[i, d],
                                                recv_sem=st_r.at[i, me],
                                                device_id=(dp, o // 4, o % 4), device_id_type=MESH)

        def stat_wait(i, d):
            o = (me + d) % 8
            return pltpu.make_async_remote_copy(src_ref=ST.at[i], dst_ref=SR.at[i, o], send_sem=st_s.at[i, d],
                                                recv_sem=st_r.at[i, o],
                                                device_id=(dp, o // 4, o % 4), device_id_type=MESH)

        def send_stats(i):
            m = state[0]
            mx = jnp.max(m, axis=0, keepdims=True)
            e = jnp.exp(m - mx)
            row = lax.broadcasted_iota(jnp.int32, (8, ROWS), 0)
            pk = jnp.broadcast_to(mx, (8, ROWS))
            for n in (1, 2, 3):
                v = state[n] * e if n < 3 else state[n]
                pk = jnp.where(row == n, jnp.sum(v, axis=0, keepdims=True), pk)
            ST[i] = pk
            SR[i, me] = pk
            for d in range(1, 8):
                stat_copy(i, d).start()

        def recv_stats(i):
            for d in range(1, 8):
                stat_wait(i, d).wait_recv()
            parts = [SR[i, o] for o in range(8)]
            mg = parts[0][0:1, :]
            for p_ in parts[1:]:
                mg = jnp.maximum(mg, p_[0:1, :])
            sg = wgt = tl = jnp.zeros((1, ROWS), f32)
            for p_ in parts:
                e = jnp.exp(p_[0:1, :] - mg)
                sg = sg + p_[1:2, :] * e
                wgt = wgt + p_[2:3, :] * e
                tl = tl + p_[3:4, :]
            lg = mg + jnp.log(sg)
            cs = pl.ds(al(i * ROWS, ROWS), ROWS)
            stats[0:1, cs] = lg
            stats[1:2, cs] = lg - wgt / sg
            stats[2:3, cs] = tl - lg
            LN[...] = jnp.broadcast_to(lg, (8, ROWS))

        def chunk(j, carry):
            rows = pl.ds(al(j * ROWS, ROWS), ROWS)
            cur, old = lax.rem(j, 2), lax.rem(j + 1, 2)
            cs = pl.ds(al(j * ROWS, ROWS), ROWS)
            IT[...] = jnp.broadcast_to(1.0 / temp[:, cs], (8, ROWS))
            tid = tgt[:, cs] - me * V
            TG[...] = jnp.broadcast_to(tid, (8, ROWS))

            def vblock(b):
                lo = 0
                for r0, n in VB[b]:
                    L[b][cur, lo:lo + n, :] = dott(W[r0:r0 + n, :], X[rows, :]) * IT[0:1, :]
                    lo += n

            for b in range(4):
                @pl.when(j == 0)
                def _():
                    for t in ((0,), (1,), (2,), (3, 4))[b]:
                        vload(t).wait()

                progress(3, j, b)
                if b == 3:
                    @pl.when(j >= 2)
                    def _():
                        for cp in ocopies(j - 2, range(4)):
                            cp.wait()

                    @pl.when(j >= 1)
                    def _():
                        recv_stats(j - 1)

                vblock(b)
                if b >= 1:
                    stats_block(cur, b - 1)
                if b == 3:
                    done = range(4)
                    for d in done:
                        final_block(old, d)

                    @pl.when(j >= 1)
                    def _():
                        for cp in ocopies(j - 1, done):
                            cp.start()

                @pl.when(j == CHUNKS - 1)
                def _():
                    for cp in lcopies(b):
                        cp.start()

            stats_block(cur, 3)
            send_stats(j)
            return carry

        lax.fori_loop(0, CHUNKS, chunk, 0)
        for i in range(CHUNKS):
            for k in range(NK):
                if k >= KA1 or i >= 2:
                    copy(i, k).wait_send()
        for cp in ocopies(CHUNKS - 2, range(4)):
            cp.wait()
        for b in range(4):
            for cp in lcopies(b):
                cp.wait()
        recv_stats(CHUNKS - 1)
        for i in range(CHUNKS):
            for d in range(1, 8):
                stat_copy(i, d).wait_send()

    pl.run_scoped(phase2, *[pltpu.VMEM((2, n, ROWS), f32) for n in VN], pltpu.VMEM((V, ROWS), bf16),
                  pltpu.VMEM((4, 8, ROWS), f32), pltpu.VMEM((8, ROWS), f32), pltpu.VMEM((8, ROWS), jnp.int32),
                  pltpu.VMEM((8, ROWS), f32), pltpu.SemaphoreType.DMA((4, 2)), pltpu.SemaphoreType.DMA((4, 2)))


def finish(lp, l, st_ref, out, s0, s1, s2, lpv, lv, ov, isem, jsem, osem, psem):
    n = lpv.shape[1]
    pieces = range(V // PIECE)

    def rows(k):
        return pl.ds(k * PIECE, PIECE)

    early = [pltpu.make_async_copy(lp.at[rows(k), pl.ds(0, n)], lpv.at[rows(k), :], isem.at[k]) for k in pieces]
    late = [pltpu.make_async_copy(l.at[rows(k), :], lv.at[rows(k), :], jsem.at[k]) for k in pieces]
    put = [pltpu.make_async_copy(lpv.at[rows(k), :], out.at[rows(k), pl.ds(0, n)], osem.at[k]) for k in pieces]
    end = [pltpu.make_async_copy(ov.at[rows(k), :], out.at[rows(k), pl.ds(n, ROWS)], psem.at[k]) for k in pieces]
    for k in pieces:
        early[k].start()
        late[k].start()
    s0[...] = st_ref[0:1, :]
    s1[...] = st_ref[1:2, :]
    s2[...] = st_ref[2:3, :]
    for k in pieces:
        early[k].wait()
        put[k].start()
        late[k].wait()
        r = k * PIECE
        ov[r:r + PIECE, :] = (lv[r:r + PIECE, :] - st_ref[0:1, n:]).astype(bf16)
        end[k].start()
    for k in pieces:
        put[k].wait()
        end[k].wait()


def solution(mesh):
    model_axes = ('tp2', 'tp')

    def local_step(hidden, w_gate, w_up, w_down, norm_gain, w_vocab, temperature, target_ids):
        n = hidden.shape[0]
        anyspec = pl.BlockSpec(memory_space=pl.ANY)
        vspec = pl.BlockSpec(memory_space=pltpu.VMEM)
        early, last_l, stats = pl.pallas_call(
            kernel,
            out_shape=(jax.ShapeDtypeStruct((V, n), bf16), jax.ShapeDtypeStruct((V, ROWS), f32),
                       jax.ShapeDtypeStruct((8, n), f32)),
            in_specs=[anyspec, anyspec, anyspec, anyspec, vspec, anyspec, vspec, vspec],
            out_specs=(anyspec, anyspec, vspec),
            scratch_shapes=[
                pltpu.VMEM((n, D), bf16),
                pltpu.VMEM((2, ROWS, D), bf16),
                pltpu.VMEM((2, ROWS // 2, D), bf16),
                pltpu.VMEM((2, 2, ROWS // 8, D), bf16),
                pltpu.VMEM((2, ROWS // 8, D), bf16),
                pltpu.VMEM((V, D), bf16),
                pltpu.VMEM((16, D), f32),
                pltpu.VMEM((CHUNKS, 8, ROWS), f32),
                pltpu.VMEM((CHUNKS, 8, 8, ROWS), f32),
                pltpu.SemaphoreType.DMA((CHUNKS, NK)),
                pltpu.SemaphoreType.DMA((CHUNKS, NK)),
                pltpu.SemaphoreType.DMA((CHUNKS, 8)),
                pltpu.SemaphoreType.DMA((CHUNKS, 8)),
                pltpu.SemaphoreType.DMA((CHUNKS,)),
                pltpu.SemaphoreType.DMA((4, 2)),
                pltpu.SemaphoreType.DMA((5,)),
                pltpu.SemaphoreType.REGULAR((3,)),
            ],
            compiler_params=pltpu.CompilerParams(collective_id=0, has_side_effects=True, vmem_limit_bytes=67043328),
        )(hidden, w_gate.T, w_up.T, w_down, norm_gain.reshape(1, D), w_vocab.T,
          temperature.reshape(1, n), target_ids.reshape(1, n))
        dma = pltpu.SemaphoreType.DMA((V // PIECE,))
        logprobs, s0, s1, s2 = pl.pallas_call(
            finish,
            out_shape=(jax.ShapeDtypeStruct((V, n), bf16),) + (jax.ShapeDtypeStruct((1, n), f32),) * 3,
            in_specs=[anyspec, anyspec, vspec],
            out_specs=(anyspec, vspec, vspec, vspec),
            scratch_shapes=[pltpu.VMEM((V, n - ROWS), bf16), pltpu.VMEM((V, ROWS), f32), pltpu.VMEM((V, ROWS), bf16),
                            dma, dma, dma, dma],
            compiler_params=pltpu.CompilerParams(vmem_limit_bytes=67043328),
        )(early, last_l, stats)
        return s0.reshape(n), s1.reshape(n), s2.reshape(n), logprobs.T

    return jax.shard_map(
        local_step, mesh=mesh,
        in_specs=(P('dp', None), P(None, model_axes), P(None, model_axes), P(model_axes, None),
                  P(None), P(None, model_axes), P('dp'), P('dp')),
        out_specs=(P('dp'), P('dp'), P('dp'), P('dp', model_axes)),
        check_vma=False)
```

```python
import functools

import jax
import jax.numpy as jnp
from jax import lax
from jax.experimental import pallas as pl
from jax.experimental.pallas import tpu as pltpu
from jax.sharding import PartitionSpec as P

NORM_EPS = 1e-6
ROWS = 256
CHUNKS = 4
D = 4096
PIECE = 400
FF = 1376
V = 4000
GB = ((0, 256), (256, 256), (512, 512), (1024, 352))
VL = ((2752, 1248), (0, 1024), (1376, 1024), (1024, 352), (2400, 352))
VB = (((2752, 624), (3376, 624)), ((0, 512), (512, 512)), ((1376, 512), (1888, 512)), ((1024, 352), (2400, 352)))
VN = (1248, 1024, 1024, 704)
VR = (((2752, 0, 1248),), ((0, 0, 1024),), ((1376, 0, 1024),), ((1024, 0, 352), (2400, 352, 352)))
f32, bf16 = jnp.float32, jnp.bfloat16
MESH = pl.DeviceIdType.MESH

B1B_LATE = False
TABLE = {
    (1, 1, 0): [('E1a', 0)],
    (1, 1, 2): [('E1b', 0)],
    (1, 1, 3): [('E2a', 0)],
    (2, 1, 1): [('E2b', 0), ('E1a', 1)],
    (1, 2, 0): [('E3', 0)],
    (1, 2, 2): [('E1b', 1)],
    (2, 2, 0): [('E2a', 1), ('E4', 0)],
    (2, 2, 1): [('E2b', 1), ('E1a', 2)],
    (1, 3, 1): [('E3', 1)],
    (2, 3, 0): [('E1b', 2), ('E5', 0)],
    (2, 3, 1): [('E2a', 2), ('E6', 0)],
    (3, 0, 0): [('E7', 0), ('E4', 1)],
    (3, 0, 1): [('E1a', 3)],
    (3, 0, 2): [('E1b', 3), ('E2b', 2), ('E5', 1)],
    (3, 0, 3): [('E6', 1), ('E3', 2)],
    (3, 1, 0): [('E7', 1)],
    (3, 1, 1): [('E2a', 3), ('E2b', 3)],
    (3, 1, 2): [('E4', 2)],
    (3, 1, 3): [('E3', 3)],
    (3, 2, 0): [('E5', 2), ('E6', 2), ('E7', 2)],
    (3, 2, 1): [('E4', 3)],
    (3, 2, 2): [('E5', 3)],
    (3, 2, 3): [('E6', 3)],
    (3, 3, 0): [('E7', 3)],
}

KD, KB1A, KB1B, KB2, KA1, KA2A, KA2B, KA3A, KA3B, KA3C, KA3D = 0, 2, 4, 6, 8, 9, 10, 11, 12, 13, 14
NK = 15


def kernel(hid, wg, wu, wd, gain, wv, temp, tgt, out, last_l, stats,
           X, PB, DR, B1, B2, W, rsc, ST, SR,
           ssem, rsem, st_s, st_r, xsem, gsem, vsem, credit):
    dp = lax.axis_index('dp')
    y = lax.axis_index('tp2')
    tpi = lax.axis_index('tp')
    x = tpi // 2
    c = tpi % 2
    me = y * 4 + tpi
    f = x + c * (y - x)
    s = y + c * (x - y)
    partner = (dp, y, x * 2 + (1 - c))
    nbr1 = (dp, y + c * (1 - 2 * y), (x + (1 - c) * (1 - 2 * x)) * 2 + c)
    nbr2 = (dp, y + (1 - c) * (1 - 2 * y), (x + c * (1 - 2 * x)) * 2 + c)
    half = c * 128

    def al(v, n):
        return pl.multiple_of(v, n)

    def q(fp, sp):
        return al((2 * fp + sp) * 32, 32)

    def xload(i):
        return pltpu.make_async_copy(hid.at[pl.ds(i * ROWS, ROWS), :], X.at[pl.ds(i * ROWS, ROWS), :], xsem.at[i])

    def gload(b, k):
        src, base = ((wg, 0), (wu, FF))[k]
        r0, n = GB[b]
        return pltpu.make_async_copy(src.at[pl.ds(r0, n), :], W.at[pl.ds(base + r0, n), :], gsem.at[b, k])

    def vload(t):
        r0, n = VL[t]
        return pltpu.make_async_copy(wv.at[pl.ds(r0, n), :], W.at[pl.ds(r0, n), :], vsem.at[t])

    def remote(src, dst, i, k, dev):
        return pltpu.make_async_remote_copy(src_ref=src, dst_ref=dst, send_sem=ssem.at[i, k], recv_sem=rsem.at[i, k],
                                            device_id=dev, device_id_type=MESH)

    def xrows(i, fp, sp, hb):
        return X.at[pl.ds(al(i * ROWS + hb + q(fp, sp), 32), 32), :]

    def prow(i, fp, sp, cs):
        return PB.at[lax.rem(i, 2), pl.ds(al(half + q(fp, sp), 32), 32), cs]

    def copy(i, k):
        sl = lax.rem(i, 2)
        if k < KA1:
            kind = k - k % 2
            cs = pl.ds(2048 * (k % 2), 2048)
            if kind == KD:
                return remote(PB.at[sl, pl.ds(al(128 - half, 128), 128), cs], DR.at[sl, :, cs], i, k, partner)
            if kind == KB1A:
                return remote(prow(i, 1 - f, 1 - s, cs), B1.at[sl, 0, :, cs], i, k, nbr1)
            if kind == KB1B:
                return remote(prow(i, 1 - f, s, cs), B1.at[sl, 1, :, cs], i, k, nbr1)
            return remote(prow(i, f, 1 - s, cs), B2.at[sl, :, cs], i, k, nbr2)
        fp, sp = {KA1: (f, s), KA2A: (f, s), KA3A: (f, s), KA2B: (f, 1 - s), KA3B: (f, 1 - s),
                  KA3C: (1 - f, s), KA3D: (1 - f, 1 - s)}[k]
        dev = {KA1: nbr2, KA2A: nbr1, KA2B: nbr1}.get(k, partner)
        r = xrows(i, fp, sp, half)
        return remote(r, r, i, k, dev)

    def e1(i, h):
        copy(i, KD + h).wait_recv()
        sl = lax.rem(i, 2)
        for sp, k in ((1 - s, KB1A), (s, KB1B)):
            r0 = q(1 - f, sp)

            def add(t, carry):
                pr = pl.ds(al(half + r0 + t * 16, 16), 16)
                dr = pl.ds(al(r0 + t * 16, 16), 16)
                for cb in range(2):
                    cs = slice(2048 * h + cb * 1024, 2048 * h + cb * 1024 + 1024)
                    PB[sl, pr, cs] = (PB[sl, pr, cs].astype(f32) + DR[sl, dr, cs].astype(f32)).astype(bf16)
                return carry

            lax.fori_loop(0, 2, add, 0)
            if k == KB1A and i >= 2 and h == 0:
                pl.semaphore_wait(credit.at[1], 1)
            if k == KB1A or not B1B_LATE:
                copy(i, k + h).start()

    def e2(i, h):
        copy(i, KB1A + h).wait_recv()
        sl = lax.rem(i, 2)
        r0 = q(f, 1 - s)

        def add(t, carry):
            pr = pl.ds(al(half + r0 + t * 16, 16), 16)
            dr = pl.ds(al(r0 + t * 16, 16), 16)
            br = pl.ds(al(t * 16, 16), 16)
            for cb in range(2):
                cs = slice(2048 * h + cb * 1024, 2048 * h + cb * 1024 + 1024)
                PB[sl, pr, cs] = (PB[sl, pr, cs].astype(f32) + DR[sl, dr, cs].astype(f32)
                                  + B1[sl, 0, br, cs].astype(f32)).astype(bf16)
            return carry

        lax.fori_loop(0, 2, add, 0)
        if i >= 2 and h == 0:
            pl.semaphore_wait(credit.at[2], 1)
        copy(i, KB2 + h).start()
        if B1B_LATE:
            copy(i, KB1B + h).start()

    def e3(i):
        for h in range(2):
            copy(i, KB1B + h).wait_recv()
            copy(i, KB2 + h).wait_recv()
        sl = lax.rem(i, 2)
        r0 = q(f, s)

        def fin(t, carry):
            pr = pl.ds(al(half + r0 + t * 16, 16), 16)
            dr = pl.ds(al(r0 + t * 16, 16), 16)
            br = pl.ds(al(t * 16, 16), 16)
            xr = pl.ds(al(i * ROWS + half + r0 + t * 16, 16), 16)
            acc = jnp.zeros((16, 128), f32)
            for cb in range(16):
                cs = slice(cb * 256, cb * 256 + 256)
                part = (PB[sl, pr, cs].astype(f32) + DR[sl, dr, cs].astype(f32)
                        + B1[sl, 1, br, cs].astype(f32) + B2[sl, br, cs].astype(f32)).astype(bf16)
                r = X[xr, cs].astype(f32) + part.astype(f32)
                rsc[:, cs] = r
                sq = r * r
                acc = acc + sq[:, :128] + sq[:, 128:]
            ms = jnp.sum(acc, axis=1, keepdims=True) * (1.0 / D)
            inv = lax.rsqrt(ms + NORM_EPS)
            for cb in range(16):
                cs = slice(cb * 256, cb * 256 + 256)
                X[xr, cs] = (gain[:, cs] * rsc[:, cs] * inv).astype(bf16)
            return carry

        lax.fori_loop(0, 2, fin, 0)
        copy(i, KA1).start()
        copy(i, KA2A).start()
        copy(i, KA3A).start()
        if i < 2:
            for n, dev in ((0, partner), (1, nbr1), (2, nbr2)):
                pl.semaphore_signal(credit.at[n], inc=1, device_id=dev, device_id_type=MESH)

    def e4(i):
        copy(i, KA1).wait_recv()
        copy(i, KA2B).start()
        copy(i, KA3B).start()

    def e5(i):
        copy(i, KA2A).wait_recv()
        copy(i, KA3C).start()

    def e6(i):
        copy(i, KA2B).wait_recv()
        copy(i, KA3D).start()

    def e7(i):
        for k in (KA3A, KA3B, KA3C, KA3D):
            copy(i, k).wait_recv()

    events = {'E3': e3, 'E4': e4, 'E5': e5, 'E6': e6, 'E7': e7}
    for h_, n_ in ((0, 'a'), (1, 'b')):
        events['E1' + n_] = functools.partial(e1, h=h_)
        events['E2' + n_] = functools.partial(e2, h=h_)

    def progress(phase, i, b):
        for ck in range(CHUNKS):
            todo = TABLE.get((phase, ck, b), [])
            if todo:
                @pl.when(i == ck)
                def _():
                    for name, cc in todo:
                        events[name](cc)

    xload(0).start()
    for b in range(2):
        for k in range(2):
            gload(b, k).start()

    def dott(w, xv):
        return lax.dot_general(w, xv, (((1,), (1,)), ((), ())), preferred_element_type=f32)

    def phase1(wdv, act, dsem):
        def dload(k):
            cs = pl.ds(2048 * k, 2048)
            return pltpu.make_async_copy(wd.at[:, cs], wdv.at[:, cs], dsem.at[k])


        bar = pltpu.get_barrier_semaphore()
        for d in range(1, 8):
            o = (me + d) % 8
            pl.semaphore_signal(bar, inc=1, device_id=(dp, o // 4, o % 4), device_id_type=MESH)
        pl.semaphore_wait(bar, 7)
        for k in range(2):
            gload(2, k).start()

        def chunk(i, carry):
            rows = pl.ds(al(i * ROWS, ROWS), ROWS)
            sl = lax.rem(i, 2)
            xload(i).wait()

            def first(fn):
                pl.when(i == 0)(fn)

            def last(fn):
                pl.when(i == CHUNKS - 1)(fn)

            for b, (r0, n) in enumerate(GB):
                @first
                def _():
                    for k in range(2):
                        gload(b, k).wait()
                    for cp in ((gload(3, 0), gload(3, 1)), (dload(0), dload(1)), (xload(1), xload(2), xload(3)), ())[b]:
                        cp.start()

                progress(1, i, b)
                g = dott(W[r0:r0 + n, :], X[rows, :])
                u = dott(W[FF + r0:FF + r0 + n, :], X[rows, :])
                h = g * jax.nn.sigmoid(g) * u
                act[:, r0:r0 + n] = jnp.transpose(h.astype(bf16))

                @last
                def _():
                    for t in ((), (), (1, 2), (3, 4))[b]:
                        vload(t).start()

            @first
            def _():
                vload(0).start()

            for b in range(2):
                first(lambda: dload(b).wait())
                progress(2, i, b)
                if b == 0:
                    @pl.when(i >= 2)
                    def _():
                        for k in range(KA1):
                            copy(i - 2, k).wait_send()
                        pl.semaphore_wait(credit.at[0], 1)

                for n in range(8):
                    cs = slice(2048 * b + 256 * n, 2048 * b + 256 * n + 256)
                    PB[sl, :, cs] = jnp.dot(act[...], wdv[:, cs], preferred_element_type=f32).astype(bf16)

                copy(i, KD + b).start()

            return carry

        lax.fori_loop(0, CHUNKS, chunk, 0)

    pl.run_scoped(phase1, pltpu.VMEM((FF, D), bf16), pltpu.VMEM((ROWS, FF), bf16), pltpu.SemaphoreType.DMA((2,)))

    def phase2(L0, L1, L2, L3, OS, state, IT, TG, LN, osem, lsem):
        L = (L0, L1, L2, L3)
        sub = lax.broadcasted_iota(jnp.int32, (8, ROWS), 0)

        def stats_block(cur, b):
            groups = [(lo + k, v + k) for v, lo, n in VR[b] for k in range(0, n, 8)]
            ms = [L[b][cur, r:r + 8, :] for r, _ in groups[:4]]
            for k, (r, _) in enumerate(groups[4:]):
                ms[k % 4] = jnp.maximum(ms[k % 4], L[b][cur, r:r + 8, :])
            m_new = jnp.maximum(jnp.maximum(ms[0], ms[1]), jnp.maximum(ms[2], ms[3]))
            zero = jnp.zeros((8, ROWS), f32)
            ss, ws, ts = [zero] * 2, [zero] * 2, [zero] * 2
            if b > 0:
                m_old = state[0]
                m_new = jnp.maximum(m_new, m_old)
                scale = jnp.exp(m_old - m_new)
                ss[0], ws[0], ts[0] = state[1] * scale, state[2] * scale, state[3]
            tg = TG[...] - sub
            for k, (r, v) in enumerate(groups):
                l = L[b][cur, r:r + 8, :]
                e = jnp.exp(l - m_new)
                ss[k % 2] = ss[k % 2] + e
                ws[k % 2] = ws[k % 2] + e * l
                ts[k % 2] = jnp.where(tg == v, l, ts[k % 2])
            state[0] = m_new
            state[1] = ss[0] + ss[1]
            state[2] = ws[0] + ws[1]
            state[3] = ts[0] + ts[1]

        def final_block(old, b):
            for v, lo, n in VR[b]:
                for k in range(0, n, 16):
                    OS[v + k:v + k + 16, :] = (L[b][old, lo + k:lo + k + 16, :] - LN[0:1, :]).astype(bf16)

        def ocopies(i, blocks):
            return [pltpu.make_async_copy(OS.at[pl.ds(v, n), :], out.at[pl.ds(v, n), pl.ds(al(i * ROWS, ROWS), ROWS)],
                                          osem.at[b, k]) for b in blocks for k, (v, lo, n) in enumerate(VR[b])]

        def lcopies(b):
            return [pltpu.make_async_copy(L[b].at[(CHUNKS - 1) % 2, pl.ds(lo, n), :], last_l.at[pl.ds(v, n), :], lsem.at[b, k])
                    for k, (v, lo, n) in enumerate(VR[b])]

        def stat_copy(i, d):
            o = (me + d) % 8
            return pltpu.make_async_remote_copy(src_ref=ST.at[i], dst_ref=SR.at[i, me], send_sem=st_s.at[i, d],
                                                recv_sem=st_r.at[i, me],
                                                device_id=(dp, o // 4, o % 4), device_id_type=MESH)

        def stat_wait(i, d):
            o = (me + d) % 8
            return pltpu.make_async_remote_copy(src_ref=ST.at[i], dst_ref=SR.at[i, o], send_sem=st_s.at[i, d],
                                                recv_sem=st_r.at[i, o],
                                                device_id=(dp, o // 4, o % 4), device_id_type=MESH)

        def send_stats(i):
            m = state[0]
            mx = jnp.max(m, axis=0, keepdims=True)
            e = jnp.exp(m - mx)
            row = lax.broadcasted_iota(jnp.int32, (8, ROWS), 0)
            pk = jnp.broadcast_to(mx, (8, ROWS))
            for n in (1, 2, 3):
                v = state[n] * e if n < 3 else state[n]
                pk = jnp.where(row == n, jnp.sum(v, axis=0, keepdims=True), pk)
            ST[i] = pk
            SR[i, me] = pk
            for d in range(1, 8):
                stat_copy(i, d).start()

        def recv_stats(i):
            for d in range(1, 8):
                stat_wait(i, d).wait_recv()
            parts = [SR[i, o] for o in range(8)]
            mg = parts[0][0:1, :]
            for p_ in parts[1:]:
                mg = jnp.maximum(mg, p_[0:1, :])
            sg = wgt = tl = jnp.zeros((1, ROWS), f32)
            for p_ in parts:
                e = jnp.exp(p_[0:1, :] - mg)
                sg = sg + p_[1:2, :] * e
                wgt = wgt + p_[2:3, :] * e
                tl = tl + p_[3:4, :]
            lg = mg + jnp.log(sg)
            cs = pl.ds(al(i * ROWS, ROWS), ROWS)
            stats[0:1, cs] = lg
            stats[1:2, cs] = lg - wgt / sg
            stats[2:3, cs] = tl - lg
            LN[...] = jnp.broadcast_to(lg, (8, ROWS))

        def chunk(j, carry):
            rows = pl.ds(al(j * ROWS, ROWS), ROWS)
            cur, old = lax.rem(j, 2), lax.rem(j + 1, 2)
            cs = pl.ds(al(j * ROWS, ROWS), ROWS)
            IT[...] = jnp.broadcast_to(1.0 / temp[:, cs], (8, ROWS))
            tid = tgt[:, cs] - me * V
            TG[...] = jnp.broadcast_to(tid, (8, ROWS))

            def vblock(b):
                lo = 0
                for r0, n in VB[b]:
                    L[b][cur, lo:lo + n, :] = dott(W[r0:r0 + n, :], X[rows, :]) * IT[0:1, :]
                    lo += n

            for b in range(4):
                @pl.when(j == 0)
                def _():
                    for t in ((0,), (1,), (2,), (3, 4))[b]:
                        vload(t).wait()

                progress(3, j, b)
                if b == 3:
                    @pl.when(j >= 2)
                    def _():
                        for cp in ocopies(j - 2, range(4)):
                            cp.wait()

                    @pl.when(j >= 1)
                    def _():
                        recv_stats(j - 1)

                vblock(b)
                if b >= 1:
                    stats_block(cur, b - 1)
                if b == 3:
                    done = range(4)
                    for d in done:
                        final_block(old, d)

                    @pl.when(j >= 1)
                    def _():
                        for cp in ocopies(j - 1, done):
                            cp.start()

                @pl.when(j == CHUNKS - 1)
                def _():
                    for cp in lcopies(b):
                        cp.start()

            stats_block(cur, 3)
            send_stats(j)
            return carry

        lax.fori_loop(0, CHUNKS, chunk, 0)
        for i in range(CHUNKS):
            for k in range(NK):
                if k >= KA1 or i >= 2:
                    copy(i, k).wait_send()
        for cp in ocopies(CHUNKS - 2, range(4)):
            cp.wait()
        for b in range(4):
            for cp in lcopies(b):
                cp.wait()
        recv_stats(CHUNKS - 1)
        for i in range(CHUNKS):
            for d in range(1, 8):
                stat_copy(i, d).wait_send()

    pl.run_scoped(phase2, *[pltpu.VMEM((2, n, ROWS), f32) for n in VN], pltpu.VMEM((V, ROWS), bf16),
                  pltpu.VMEM((4, 8, ROWS), f32), pltpu.VMEM((8, ROWS), f32), pltpu.VMEM((8, ROWS), jnp.int32),
                  pltpu.VMEM((8, ROWS), f32), pltpu.SemaphoreType.DMA((4, 2)), pltpu.SemaphoreType.DMA((4, 2)))


def finish(lp, l, st_ref, out, s0, s1, s2, lpv, lv, ov, isem, jsem, osem, psem):
    n = lpv.shape[1]
    pieces = range(V // PIECE)

    def rows(k):
        return pl.ds(k * PIECE, PIECE)

    early = [pltpu.make_async_copy(lp.at[rows(k), pl.ds(0, n)], lpv.at[rows(k), :], isem.at[k]) for k in pieces]
    late = [pltpu.make_async_copy(l.at[rows(k), :], lv.at[rows(k), :], jsem.at[k]) for k in pieces]
    put = [pltpu.make_async_copy(lpv.at[rows(k), :], out.at[rows(k), pl.ds(0, n)], osem.at[k]) for k in pieces]
    end = [pltpu.make_async_copy(ov.at[rows(k), :], out.at[rows(k), pl.ds(n, ROWS)], psem.at[k]) for k in pieces]
    for k in pieces:
        early[k].start()
        late[k].start()
    s0[...] = st_ref[0:1, :]
    s1[...] = st_ref[1:2, :]
    s2[...] = st_ref[2:3, :]
    for k in pieces:
        early[k].wait()
        put[k].start()
        late[k].wait()
        r = k * PIECE
        ov[r:r + PIECE, :] = (lv[r:r + PIECE, :] - st_ref[0:1, n:]).astype(bf16)
        end[k].start()
    for k in pieces:
        put[k].wait()
        end[k].wait()


def solution(mesh):
    model_axes = ('tp2', 'tp')

    def local_step(hidden, w_gate, w_up, w_down, norm_gain, w_vocab, temperature, target_ids):
        n = hidden.shape[0]
        anyspec = pl.BlockSpec(memory_space=pl.ANY)
        vspec = pl.BlockSpec(memory_space=pltpu.VMEM)
        early, last_l, stats = pl.pallas_call(
            kernel,
            out_shape=(jax.ShapeDtypeStruct((V, n), bf16), jax.ShapeDtypeStruct((V, ROWS), f32),
                       jax.ShapeDtypeStruct((8, n), f32)),
            in_specs=[anyspec, anyspec, anyspec, anyspec, vspec, anyspec, vspec, vspec],
            out_specs=(anyspec, anyspec, vspec),
            scratch_shapes=[
                pltpu.VMEM((n, D), bf16),
                pltpu.VMEM((2, ROWS, D), bf16),
                pltpu.VMEM((2, ROWS // 2, D), bf16),
                pltpu.VMEM((2, 2, ROWS // 8, D), bf16),
                pltpu.VMEM((2, ROWS // 8, D), bf16),
                pltpu.VMEM((V, D), bf16),
                pltpu.VMEM((16, D), f32),
                pltpu.VMEM((CHUNKS, 8, ROWS), f32),
                pltpu.VMEM((CHUNKS, 8, 8, ROWS), f32),
                pltpu.SemaphoreType.DMA((CHUNKS, NK)),
                pltpu.SemaphoreType.DMA((CHUNKS, NK)),
                pltpu.SemaphoreType.DMA((CHUNKS, 8)),
                pltpu.SemaphoreType.DMA((CHUNKS, 8)),
                pltpu.SemaphoreType.DMA((CHUNKS,)),
                pltpu.SemaphoreType.DMA((4, 2)),
                pltpu.SemaphoreType.DMA((5,)),
                pltpu.SemaphoreType.REGULAR((3,)),
            ],
            compiler_params=pltpu.CompilerParams(collective_id=0, has_side_effects=True, vmem_limit_bytes=67043328),
        )(hidden, w_gate.T, w_up.T, w_down, norm_gain.reshape(1, D), w_vocab.T,
          temperature.reshape(1, n), target_ids.reshape(1, n))
        dma = pltpu.SemaphoreType.DMA((V // PIECE,))
        logprobs, s0, s1, s2 = pl.pallas_call(
            finish,
            out_shape=(jax.ShapeDtypeStruct((V, n), bf16),) + (jax.ShapeDtypeStruct((1, n), f32),) * 3,
            in_specs=[anyspec, anyspec, vspec],
            out_specs=(anyspec, vspec, vspec, vspec),
            scratch_shapes=[pltpu.VMEM((V, n - ROWS), bf16), pltpu.VMEM((V, ROWS), f32), pltpu.VMEM((V, ROWS), bf16),
                            dma, dma, dma, dma],
            compiler_params=pltpu.CompilerParams(vmem_limit_bytes=67043328),
        )(early, last_l, stats)
        return s0.reshape(n), s1.reshape(n), s2.reshape(n), logprobs.T

    return jax.shard_map(
        local_step, mesh=mesh,
        in_specs=(P('dp', None), P(None, model_axes), P(None, model_axes), P(model_axes, None),
                  P(None), P(None, model_axes), P('dp'), P('dp')),
        out_specs=(P('dp'), P('dp'), P('dp'), P('dp', model_axes)),
        check_vma=False)
```
